32 devices in a mesh: grp: 8 (over z, x), sub: 4 (over y, core).
Axes of the slice: x: 2, y: 2, z: 4, core: 2. Of those that a mesh axis runs over, the one named last changes fastest.
Arguments:
- residual: float32 [98304], P(('grp', 'sub')), may hold values from -6 to 6
- edge_scale: float32 [98304], P(('grp', 'sub')), may hold values from 0.2 to 1
- tangent: float32 [3, 98304], P(None, ('grp', 'sub')), may hold values from -6 to 6
- edge_tail: int32 [98304], P(('grp', 'sub')), may hold values from 0 to 511
- edge_head: int32 [98304], P(('grp', 'sub')), may hold values from 0 to 4607
- stencil_index: int32 [14, 16384], P(None, ('grp', 'sub')), may hold values from 0 to 4607
- stencil_coef: bfloat16 [4, 14, 16384], P(None, None, ('grp', 'sub')), may hold values from -1 to -0.099609375
- diag_margin: float32 [4, 16384], P(None, ('grp', 'sub')), may hold values from 0.05 to 0.5
- send_index: int32 [16, 8, 512], P('grp', 'sub'), may hold values from 0 to 511
Outputs:
- correction: float32 [98304], P(('grp', 'sub'))
The draws below stay inside these ranges and needn't reach their ends.
Inputs may be any that keep to these rules, and one draw needn't show every extreme that they name: `edge_tail`: positions among a device's own nodes. `edge_head`: positions in the device's extended list: own nodes first, then the 8 received blocks. `stencil_index`: positions in the extended list of the device that holds the row. `send_index`: positions among the device's own nodes; an entry may repeat.
All inputs are finite; a program needn't handle non-finite values.
Results may differ from the reference program's by a relative error of at most 0.0003.
Values sent between devices are 32-bit elements; how exact they have to be, the bound alone decides.
A program may use at most 64 MiB of HBM per device.

```python
import math
import jax
import jax.numpy as jnp

N_DEV = 512
E_DEV = 3072
HALO = 512
STENCIL = 14
SWEEPS = 4
NODES = 16384
EDGES = 98304
N_GRP = 8
N_SUB = 4


def with_ends(entries, stream_key, smallest, top_value):
    longest = entries.shape.index(max(entries.shape))
    spots = []
    for shift in (0, 1):
        where = [jax.random.randint(jax.random.fold_in(stream_key, axis), (), 0, length) for axis, length in enumerate(entries.shape)]
        where[longest] = (where[longest] + shift) % entries.shape[longest]
        spots.append(tuple(where))
    return entries.at[spots[0]].set(smallest).at[spots[1]].set(top_value)


def steps_of(stream_key, extent, pieces, smallest, largest):
    factor_of, own = 1.0, jax.random.fold_in(stream_key, 6)
    for dim, shards_of in pieces:
        draws = jnp.exp(jax.random.uniform(jax.random.fold_in(own, dim), (shards_of,), jnp.float32, smallest / len(pieces), largest / len(pieces)))
        factor_of = factor_of * jnp.repeat(draws, extent[dim] // shards_of).reshape([-1 if axis == dim else 1 for axis in range(len(extent))])
    return factor_of


def scatter_about(key, shape, scale, bound, cuts=(), kind=jnp.bfloat16):
    drawn = jax.random.normal(key, shape, jnp.float32) * scale
    if len(cuts) > 0:
        drawn = steps_of(key, shape, cuts, -0.22, 0.18) * drawn
    return jnp.clip(drawn, min=-bound, max=bound).astype(kind)


def setup_inputs(seed: int = 0) -> dict:
    arg_keys = jax.random.split(jax.random.key(seed), 10)
    return {
        "residual": scatter_about(arg_keys[0], (EDGES,), 1.0, 6.0, ((0, 32),), jnp.float32),
        "edge_scale": jnp.clip(jnp.exp(math.log(1.0) - 1.609438 * jax.random.uniform(arg_keys[1], (EDGES,), jnp.float32) ** steps_of(arg_keys[1], (EDGES,), ((0, 32),), -0.2, 0.2)), 0.2, 1.0),
        "tangent": scatter_about(arg_keys[2], (3, EDGES), 1.0, 6.0, ((1, 32),), jnp.float32),
        "edge_tail": with_ends(jax.random.randint(arg_keys[3], (EDGES,), 0, N_DEV), jax.random.fold_in(arg_keys[3], 1), 0, N_DEV - 1).astype(jnp.int32),
        "edge_head": with_ends(jax.random.randint(arg_keys[4], (EDGES,), 0, N_DEV + 8 * HALO), jax.random.fold_in(arg_keys[4], 1), 0, (N_DEV + 8 * HALO) - 1).astype(jnp.int32),
        "stencil_index": with_ends(jax.random.randint(arg_keys[5], (STENCIL, NODES), 0, N_DEV + 8 * HALO), jax.random.fold_in(arg_keys[5], 1), 0, (N_DEV + 8 * HALO) - 1).astype(jnp.int32),
        "stencil_coef": jnp.clip(-1.0 + 0.9003906 * jax.random.uniform(arg_keys[6], (4, STENCIL, NODES), jnp.float32) ** steps_of(arg_keys[6], (4, STENCIL, NODES), ((2, 32),), -0.2, 0.2), -1.0, -0.099609375).astype(jnp.bfloat16),
        "diag_margin": jnp.clip(jnp.exp(math.log(0.5) - 2.3025851 * jax.random.uniform(arg_keys[7], (4, NODES), jnp.float32) ** steps_of(arg_keys[7], (4, NODES), ((1, 32),), -0.2, 0.2)), 0.05, 0.5),
        "send_index": with_ends(jax.random.randint(arg_keys[8], (2 * N_GRP, 2 * N_SUB, HALO), 0, N_DEV), jax.random.fold_in(arg_keys[8], 1), 0, N_DEV - 1).astype(jnp.int32),
    }


def ghost_table(send_index):
    blocks = send_index.reshape(N_GRP, 2, N_SUB, 2, HALO).transpose(0, 2, 1, 3, 4)
    owner_base = (jnp.arange(N_GRP * N_SUB, dtype=jnp.int32) * N_DEV).reshape(N_GRP, N_SUB, 1, 1, 1)
    global_ids = blocks + owner_base
    from_below = jnp.roll(global_ids, 1, axis=0)[:, :, 1]
    from_above = jnp.roll(global_ids, -1, axis=0)[:, :, 0]
    from_prev = jnp.roll(global_ids, 1, axis=1)[:, :, :, 1]
    from_next = jnp.roll(global_ids, -1, axis=1)[:, :, :, 0]
    ghosts = jnp.concatenate([from_below, from_above, from_prev, from_next], axis=2)
    ghosts = ghosts.reshape(N_GRP * N_SUB, 8 * HALO)
    own_ids = jnp.arange(N_GRP * N_SUB * N_DEV, dtype=jnp.int32).reshape(N_GRP * N_SUB, N_DEV)
    return jnp.concatenate([own_ids, ghosts], axis=1).reshape(-1)


def to_global(flat_table, local, per_device):
    extended = N_DEV + 8 * HALO
    device = (jnp.arange(local.shape[-1], dtype=jnp.int32) // per_device).astype(jnp.int32)
    return flat_table[device * extended + local.astype(jnp.int32)]


def reference(residual, edge_scale, tangent, edge_tail, edge_head, stencil_index, stencil_coef, diag_margin, send_index):
    flat_table = ghost_table(send_index)
    tail_ids = to_global(flat_table, edge_tail, E_DEV)
    head_ids = to_global(flat_table, edge_head, E_DEV)
    node_total = N_DEV * N_GRP * N_SUB
    half_terms = 0.5 * tangent * residual[None, :]
    vals_tail = jnp.concatenate([-residual[None, :], half_terms], axis=0)
    vals_head = jnp.concatenate([residual[None, :], half_terms], axis=0)
    node_sums = jnp.zeros((4, node_total), jnp.float32)
    node_sums = node_sums.at[:, tail_ids].add(vals_tail).at[:, head_ids].add(vals_head)
    neighbour_ids = [to_global(flat_table, stencil_index[column], N_DEV) for column in range(STENCIL)]
    diag_vals = jnp.zeros((4, node_total), jnp.float32)
    for column in range(STENCIL):
        diag_vals = diag_vals + jnp.abs(stencil_coef[:, column].astype(jnp.float32))
    diag_vals = (1.0 + diag_margin) * diag_vals
    solved = node_sums / diag_vals
    for sweep in range(SWEEPS - 1):
        applied = diag_vals * solved
        for column in range(STENCIL):
            applied = applied + stencil_coef[:, column].astype(jnp.float32) * solved[:, neighbour_ids[column]]
        solved = solved + (node_sums - applied) / diag_vals
    at_tail = solved[:, tail_ids]
    at_head = solved[:, head_ids]
    return edge_scale * residual + (at_head[0] - at_tail[0]) + 0.5 * jnp.sum(tangent * (at_tail[1:] + at_head[1:]), axis=0)
```

```python
import jax
import jax.numpy as jnp
from jax import lax
from jax.experimental import pallas as pl
from jax.experimental.pallas import tpu as pltpu
from jax.sharding import PartitionSpec as P

SWEEPS = 4
LANES = 128
SLOTS = 8
MESH = pl.DeviceIdType.MESH
DNUMS = lax.GatherDimensionNumbers(
    offset_dims=(),
    collapsed_slice_dims=(1,),
    start_index_map=(1,),
    operand_batching_dims=(0,),
    start_indices_batching_dims=(0,),
)
F32 = jnp.float32
BF16 = jnp.bfloat16
I32 = jnp.int32

OWN, FAR, NEAR, SM, SP = range(5)
FAR_NEAR, FAR_SM, FAR_SP = 5, 6, 7
GHOST_SLOT = (FAR, OWN, FAR_NEAR, FAR_SM, FAR_SP)


def lane_gather(table, lane):
    return lax.gather(
        table,
        lane[..., None],
        DNUMS,
        slice_sizes=(1, 1),
        mode=lax.GatherScatterMode.PROMISE_IN_BOUNDS,
    )


def nt_dot(a, b):
    return lax.dot_general(a, b, (((1,), (1,)), ((), ())), preferred_element_type=F32)


def kernel(
    res_h, tan_h, tail_h, head_h, sidx_h, coef_h, marg_h, send_h, scale_h,
    out_ref,
    res, tan, tail, head, sidx, coef, marg, own_send, scale,
    got_send, psend, got_p, tab, onehot, spread_o, spread_f, spread_r, onehot3, spread3, tsum,
    cf, gcf, bsc, diag, hq, hl, sq, gq, tan2,
    local_sem, send_sem, recv_sem, tab_send, tab_recv, ghost_send, ghost_recv,
):
    G, S = lax.axis_size("grp"), lax.axis_size("sub")
    g, s = lax.axis_index("grp"), lax.axis_index("sub")
    odd = lax.rem(g, 2)
    even = 1 - odd
    gf, gn = lax.rem(g + G - 1 + 2 * odd, G), lax.rem(g + 1 + (G - 2) * odd, G)
    sm, sp = lax.rem(s + S - 1, S), lax.rem(s + 1, S)
    peer = {FAR: (gf, s), NEAR: (gn, s), SM: (g, sm), SP: (g, sp)}
    nn_to = (lax.rem(g + 2 + (G - 4) * odd, G), s)
    nn_from = (lax.rem(g + G - 2 + 4 * odd, G), s)
    greeted = [peer[FAR], peer[NEAR], peer[SM], peer[SP], nn_to, nn_from, (gf, sm), (gf, sp)]
    back = {FAR: FAR, NEAR: NEAR, SM: SP, SP: SM}
    nrow = marg.shape[1] // LANES
    erow = res.shape[0]
    stencil = sidx.shape[0]
    vrow = 4 * nrow
    sent = 2 * vrow
    srows = sq.shape[0] // 8

    barrier = pltpu.get_barrier_semaphore()
    for who in greeted:
        pl.semaphore_signal(barrier, inc=1, device_id=who, device_id_type=MESH)
    pairs = (
        (head_h, head), (res_h, res), (tan_h, tan), (send_h, own_send), (tail_h, tail),
        (coef_h, coef), (marg_h, marg), (sidx_h, sidx), (scale_h, scale),
    )
    local = [
        pltpu.make_async_copy(src, dst, local_sem.at[i]) for i, (src, dst) in enumerate(pairs)
    ]
    for c in local:
        c.start()

    started = []

    def remote(src, dst, ssem, rsem, who):
        copy = pltpu.make_async_remote_copy(
            src_ref=src, dst_ref=dst, send_sem=ssem, recv_sem=rsem, device_id=who, device_id_type=MESH,
        )
        copy.start()
        started.append(copy)

    def landed(dst, rsem):
        pltpu.make_async_remote_copy(
            src_ref=dst, dst_ref=dst, send_sem=rsem, recv_sem=rsem, device_id=peer[SP], device_id_type=MESH,
        ).wait_recv()

    def part_rows(ref, o):
        return ref.at[pl.ds((o - 1) * sent, sent)]

    def send_part(o):
        remote(part_rows(psend, o), part_rows(got_p, back[o]), send_sem.at[0, o - 1], recv_sem.at[0, back[o] - 1], peer[o])

    def send_list(o):
        remote(own_send, got_send.at[back[o] - 1], send_sem.at[1, o - 1], recv_sem.at[1, back[o] - 1], peer[o])

    def slot_rows(rnd, slot):
        return tab.at[rnd, pl.ds(slot * vrow, vrow)]

    def send_table(rnd, who, slot):
        remote(slot_rows(rnd, OWN), slot_rows(rnd, slot), tab_send.at[rnd, slot - 1], tab_recv.at[rnd, slot - 1], who)

    def table_here(rnd, slot):
        landed(slot_rows(rnd, slot), tab_recv.at[rnd, slot - 1])

    riota = lax.broadcasted_iota(I32, (vrow, LANES), 0)
    kind = riota // nrow
    rpart = (riota - kind * nrow).astype(F32).astype(BF16)
    lane16 = lax.broadcasted_iota(I32, (16, LANES), 0).astype(F32).astype(BF16)
    one, zero = jnp.ones((), BF16), jnp.zeros((), BF16)

    def cols_of(t):
        return slice(t * LANES, (t + 1) * LANES)

    def wide(row, rows):
        return jnp.broadcast_to(row.astype(F32), (rows, LANES)).astype(BF16)

    def lanes_onehot(ref, cols, x):
        lane = wide(x & (LANES - 1), 16)
        for q in range(LANES // 16):
            mine = lane16 + jnp.full((), 16 * q, BF16)
            ref[q * 16 : q * 16 + 16, cols] = jnp.where(mine == lane, one, zero)

    def split(val):
        hi = val.astype(BF16)
        return hi, (val - hi.astype(F32)).astype(BF16)

    def terms(t, sign):
        r = res[t : t + 1, :]
        val = jnp.broadcast_to(r if sign > 0 else -r, (vrow, LANES))
        half = 0.5 * r
        for c in range(3):
            val = jnp.where(kind == c + 1, tan[c : c + 1, cols_of(t)] * half, val)
        return split(val)

    def scatter(ref, rows_of, bases, sign, make=None):
        n = len(bases)
        for t in range(erow):
            cols = cols_of(t)
            x = rows_of[t : t + 1, :]
            if make:
                lanes_onehot(onehot, cols, x)
            pieces = terms(t, sign)
            row = wide(x >> 7, vrow)
            for j, base in enumerate(bases):
                hit = row == rpart + base
                for p, v in enumerate(pieces):
                    at = (p * n + j) * vrow
                    ref[at : at + vrow, cols] = jnp.where(hit, v, zero)
        both = nt_dot(ref[...], onehot[...])
        return both[: n * vrow] + both[n * vrow :]

    def base_of(block):
        return (jnp.asarray(block, I32) * nrow).astype(F32).astype(BF16)

    far_block, near_block = 1 + 2 * odd, 3 - 2 * odd

    for c in local[:3]:
        c.wait()
    psend[0:sent] = scatter(spread_f, head, [base_of(far_block), base_of(far_block + 1)], 1, make=True)
    pl.semaphore_wait(barrier, len(greeted))
    send_part(FAR)
    rest = scatter(
        spread_r, head,
        [base_of(b) for b in (near_block, near_block + 1, 5, 6, 7, 8, 0)], 1,
    )
    psend[sent:] = rest[: 3 * sent]
    own_sum = rest[3 * sent :]
    for o in (NEAR, SM, SP):
        send_part(o)
    local[3].wait()
    for o in (FAR, NEAR, SM, SP):
        send_list(o)
    for c in local[4:]:
        c.wait()

    cf[...] = jnp.zeros_like(cf)
    for k in range(4):
        for r in range(nrow):
            cols = cols_of(r)
            c = coef[:, k, cols].astype(F32)
            d = (1.0 + marg[k : k + 1, cols]) * jnp.sum(jnp.abs(c), axis=0, keepdims=True)
            inv = 1.0 / d
            diag[k * nrow + r : k * nrow + r + 1, :] = inv
            cf[k, :stencil, cols] = c * inv
    remote(cf, gcf, ghost_send.at[0], ghost_recv.at[0], peer[FAR])

    for t in range(erow):
        lanes_onehot(onehot, cols_of(t), tail[t : t + 1, :])
    own_sum = own_sum + scatter(spread_o, tail, [base_of(0)], -1)

    a_of = (odd, even)
    lists = tuple((f, b, r) for f in range(2) for b in range(2) for r in range(nrow))

    def own_list(f, b, r):
        return own_send[a_of[f], b : b + 1, cols_of(r)]

    for n, fbr in enumerate(lists):
        lanes_onehot(onehot3, cols_of(n), own_list(*fbr))
    for c in range(3):
        for t in range(erow):
            tan2[c * erow + t : c * erow + t + 1, :] = tan[c : c + 1, cols_of(t)]
    sq[...] = jnp.zeros_like(sq)
    sq[:stencil, :] = sidx[...]

    def place(ref, at, f, b, r):
        hit = wide(own_list(f, b, r) >> 7, vrow) == rpart
        base = b * vrow + r + at
        val = jnp.broadcast_to(ref[base : base + 1, :], (vrow, LANES))
        for k in range(1, 4):
            row = base + k * nrow
            val = jnp.where(kind == k, ref[row : row + 1, :], val)
        return [jnp.where(hit, v, zero) for v in split(val)]

    for o in (SP, SM, NEAR):
        landed(part_rows(got_p, o), recv_sem.at[0, o - 1])
    for f in range(2):
        for b in range(2):
            first = pl.multiple_of((2 + b) * sent + a_of[f] * vrow, vrow)
            val = got_p[pl.ds(first, vrow), :]
            if f:
                val = val + got_p[sent + b * vrow : sent + (b + 1) * vrow, :]
            at = (f * 2 + b) * vrow
            tsum[at : at + vrow, :] = val
    for n, (f, b, r) in enumerate(lists):
        for p, v in enumerate(place(tsum, f * sent, f, b, r)):
            spread3[p * vrow : (p + 1) * vrow, cols_of(n)] = v
    got = nt_dot(spread3[...], onehot3[...])
    own_sum = own_sum + (got[:vrow] + got[vrow:])

    landed(part_rows(got_p, FAR), recv_sem.at[0, FAR - 1])
    half = len(lists) // 2
    for n, (f, b, r) in enumerate(lists[:half]):
        for p, v in enumerate(place(got_p, 0, f, b, r)):
            spread3[p * vrow : (p + 1) * vrow, cols_of(n)] = v
    got = nt_dot(spread3[:, : half * LANES], onehot3[:, : half * LANES])
    bsc[...] = (own_sum + (got[:vrow] + got[vrow:])) * diag[...]
    tab[0, :vrow, :] = bsc[...]

    def send_round(rnd, deep):
        if deep:
            send_table(rnd, peer[FAR], FAR)
            send_table(rnd, (gf, sp), FAR_SM)
            send_table(rnd, (gf, sm), FAR_SP)
            send_table(rnd, nn_to, FAR_NEAR)
        for o in (NEAR, SM, SP):
            send_table(rnd, peer[o], back[o])

    def compose(x):
        lane = x & (LANES - 1)
        row = x >> 7
        y = x
        for o in (FAR, NEAR, SM, SP):
            block = {FAR: far_block, NEAR: near_block, SM: 5, SP: 7}[o]
            for h in range(2):
                a, b = {FAR: (even, h), NEAR: (odd, h), SM: (h, 1), SP: (h, 0)}[o]
                for r in range(nrow):
                    line = got_send[o - 1, a, b : b + 1, cols_of(r)]
                    line = jnp.broadcast_to(line + o * nrow * LANES, x.shape)
                    y = jnp.where(row == (block + h) * nrow + r, lane_gather(line, lane), y)
        return y

    def compose_all():
        for o in (SP, SM, NEAR, FAR):
            landed(got_send.at[o - 1], recv_sem.at[1, o - 1])
        for i in range(srows):
            for r in range(nrow):
                sq[i * 8 : i * 8 + 8, cols_of(r)] = compose(sq[i * 8 : i * 8 + 8, cols_of(r)])
        remote(sq, gq, ghost_send.at[1], ghost_recv.at[1], peer[FAR])

    def compose_heads():
        for i in range(erow // 8):
            y = compose(head[i * 8 : i * 8 + 8, :])
            hq[i * 8 : i * 8 + 8, :] = y >> 7
            hl[i * 8 : i * 8 + 8, :] = y & (LANES - 1)

    def add_rows(rnd, slot, part, rows, lanes, accs):
        for i in range(len(rows)):
            for r in range(nrow):
                hit = rows[i] == part * nrow + r
                for k in range(4):
                    at = slot * vrow + k * nrow + r
                    line = jnp.broadcast_to(tab[rnd, at : at + 1, :], rows[i].shape)
                    v = lane_gather(line, lanes[i])
                    accs[i][k] = v if accs[i][k] is None else jnp.where(hit, v, accs[i][k])

    sub8 = lax.broadcasted_iota(I32, (8, LANES), 0)

    def fold(vecs):
        step = len(vecs) // 2
        while step:
            keep = (sub8 & step) == 0
            vecs = [
                jnp.where(keep, x, y) + pltpu.roll(jnp.where(keep, y, x), step, axis=0)
                if step == 4 else
                jnp.where(keep, x + pltpu.roll(x, 8 - step, axis=0), y + pltpu.roll(y, step, axis=0))
                for x, y in zip(vecs[:step], vecs[step:])
            ]
            step //= 2
        return vecs[0]

    tiles = [(slice(i * 8, i * 8 + 8), cols_of(r)) for i in range(srows) for r in range(nrow)]

    def sweep(rnd, index, factor, slots, start, out_slot, order, wait):
        where = [index[w] for w in tiles]
        rows = [y >> 7 for y in where]
        lanes = [y & (LANES - 1) for y in where]
        accs = [[None] * 4 for _ in tiles]
        for part in order:
            if part in wait:
                table_here(rnd, slots[part])
            add_rows(rnd, slots[part], part, rows, lanes, accs)
        totals = []
        for k in range(4):
            for r in range(nrow):
                total = None
                for i in range(srows):
                    n = i * nrow + r
                    v = accs[n][k] * factor[(k,) + tiles[n]]
                    total = v if total is None else total + v
                totals.append(total)
        for at in range(0, vrow, 8):
            to = out_slot * vrow + at
            tab[rnd + 1, to : to + 8, :] = start(at) - fold(totals[at : at + 8])

    def own_start(at):
        return bsc[at : at + 8, :]

    def ghost_start(at):
        return tab[0, FAR * vrow + at : FAR * vrow + at + 8, :]

    own_slots = (OWN, FAR, NEAR, SM, SP)
    for rnd in range(SWEEPS):
        deep = rnd % 2 == 0
        send_round(rnd, deep)
        if rnd == 0:
            compose_all()
        elif rnd == 1:
            compose_heads()
        if deep:
            sweep(rnd, sq, cf, own_slots, own_start, OWN, (OWN, SP, SM, NEAR, FAR), (SP, SM, NEAR, FAR))
        else:
            for slot in (FAR_NEAR, FAR_SM, FAR_SP):
                table_here(rnd - 1, slot)
            if rnd == 1:
                landed(gcf, ghost_recv.at[0])
                landed(gq, ghost_recv.at[1])
            sweep(rnd - 1, gq, gcf, GHOST_SLOT, ghost_start, FAR, (FAR, OWN, NEAR, SM, SP), ())
            if rnd < SWEEPS - 1:
                sweep(rnd, sq, cf, own_slots, own_start, OWN, (OWN, FAR, SP, SM, NEAR), (SP, SM, NEAR))

    last = SWEEPS - 1
    where = [slice(i * 8, i * 8 + 8) for i in range(erow // 8)]
    tails = [tail[w, :] for w in where]
    tacc = [[None] * 4 for _ in where]
    add_rows(last, OWN, OWN, [t >> 7 for t in tails], [t & (LANES - 1) for t in tails], tacc)
    rows = [hq[w, :] for w in where]
    lanes = [hl[w, :] for w in where]
    hacc = [[None] * 4 for _ in where]
    for part in (OWN, FAR, SP, SM, NEAR):
        if part in (SP, SM, NEAR):
            table_here(last, part)
        add_rows(last, part, part, rows, lanes, hacc)
    for i, w in enumerate(where):
        mixed = None
        for c in range(3):
            v = tan2[c * erow + i * 8 : c * erow + i * 8 + 8, :] * (tacc[i][c + 1] + hacc[i][c + 1])
            mixed = v if mixed is None else mixed + v
        out_ref[w, :] = scale[w, :] * res[w, :] + ((hacc[i][0] - tacc[i][0]) + 0.5 * mixed)

    for copy in started:
        copy.wait_send()


def body(
    residual, edge_scale, tangent, edge_tail, edge_head,
    stencil_index, stencil_coef, diag_margin, send_index,
):
    edges = residual.shape[0]
    erow = edges // LANES
    nodes = diag_margin.shape[1]
    nrow = nodes // LANES
    vrow = 4 * nrow
    stencil = stencil_index.shape[0]
    spad = -(-stencil // 8) * 8
    assert send_index.shape == (2, 2, nodes) and lax.axis_size("grp") % 2 == 0
    coef = jnp.transpose(stencil_coef, (1, 0, 2))
    square = lambda x: x.reshape(erow, LANES)
    anyspace = pl.BlockSpec(memory_space=pl.ANY)
    vm = pltpu.VMEM
    dma = pltpu.SemaphoreType.DMA
    out = pl.pallas_call(
        kernel,
        out_shape=vm((erow, LANES), F32),
        in_specs=[anyspace] * 9,
        out_specs=pl.BlockSpec(memory_space=vm),
        scratch_shapes=[
            vm((erow, LANES), F32),
            vm(tangent.shape, F32),
            vm((erow, LANES), I32),
            vm((erow, LANES), I32),
            vm(stencil_index.shape, I32),
            vm(coef.shape, BF16),
            vm(diag_margin.shape, F32),
            vm(send_index.shape, I32),
            vm((erow, LANES), F32),
            vm((4,) + send_index.shape, I32),
            vm((8 * vrow, LANES), F32),
            vm((8 * vrow, LANES), F32),
            vm((SWEEPS, SLOTS * vrow, LANES), F32),
            vm((LANES, edges), BF16),
            vm((2 * vrow, edges), BF16),
            vm((4 * vrow, edges), BF16),
            vm((14 * vrow, edges), BF16),
            vm((LANES, 4 * nodes), BF16),
            vm((2 * vrow, 4 * nodes), BF16),
            vm((4 * vrow, LANES), F32),
            vm((4, spad, nodes), F32),
            vm((4, spad, nodes), F32),
            vm((vrow, LANES), F32),
            vm((vrow, LANES), F32),
            vm((erow, LANES), I32),
            vm((erow, LANES), I32),
            vm((spad, nodes), I32),
            vm((spad, nodes), I32),
            vm((3 * erow, LANES), F32),
            dma((9,)),
            dma((2, 4)),
            dma((2, 4)),
            dma((SWEEPS, SLOTS - 1)),
            dma((SWEEPS, SLOTS - 1)),
            dma((2,)),
            dma((2,)),
        ],
        compiler_params=pltpu.CompilerParams(collective_id=0, has_side_effects=True),
    )(
        square(residual), tangent, square(edge_tail), square(edge_head),
        stencil_index, coef, diag_margin, send_index, square(edge_scale),
    )
    return out.reshape(edges)


def solution(mesh):
    return jax.shard_map(
        body,
        mesh=mesh,
        in_specs=(
            P(("grp", "sub")),
            P(("grp", "sub")),
            P(None, ("grp", "sub")),
            P(("grp", "sub")),
            P(("grp", "sub")),
            P(None, ("grp", "sub")),
            P(None, None, ("grp", "sub")),
            P(None, ("grp", "sub")),
            P("grp", "sub", None),
        ),
        out_specs=P(("grp", "sub")),
        check_vma=False,
    )
```

```python
import jax
import jax.numpy as jnp
from jax import lax
from jax.experimental import pallas as pl
from jax.experimental.pallas import tpu as pltpu
from jax.sharding import PartitionSpec as P

SWEEPS = 4
LANES = 128
SLOTS = 8
MESH = pl.DeviceIdType.MESH
DNUMS = lax.GatherDimensionNumbers(
    offset_dims=(),
    collapsed_slice_dims=(1,),
    start_index_map=(1,),
    operand_batching_dims=(0,),
    start_indices_batching_dims=(0,),
)
F32 = jnp.float32
BF16 = jnp.bfloat16
I32 = jnp.int32

OWN, FAR, NEAR, SM, SP = range(5)
FAR_NEAR, FAR_SM, FAR_SP = 5, 6, 7
GHOST_SLOT = (FAR, OWN, FAR_NEAR, FAR_SM, FAR_SP)


def lane_gather(table, lane):
    return lax.gather(
        table,
        lane[..., None],
        DNUMS,
        slice_sizes=(1, 1),
        mode=lax.GatherScatterMode.PROMISE_IN_BOUNDS,
    )


def nt_dot(a, b):
    return lax.dot_general(a, b, (((1,), (1,)), ((), ())), preferred_element_type=F32)


def kernel(
    res_h, tan_h, tail_h, head_h, sidx_h, coef_h, marg_h, send_h, scale_h,
    out_ref,
    res, tan, tail, head, sidx, coef, marg, own_send, scale,
    got_send, psend, got_p, tab, onehot, spread_o, spread_f, spread_r, onehot3, spread3, tsum,
    cf, gcf, bsc, diag, hq, hl, sq, gq, tan2,
    send_sem, recv_sem,
):
    G, S = lax.axis_size("grp"), lax.axis_size("sub")
    g, s = lax.axis_index("grp"), lax.axis_index("sub")
    odd = lax.rem(g, 2)
    even = 1 - odd
    gf, gn = lax.rem(g + G - 1 + 2 * odd, G), lax.rem(g + 1 + (G - 2) * odd, G)
    sm, sp = lax.rem(s + S - 1, S), lax.rem(s + 1, S)
    peer = {FAR: (gf, s), NEAR: (gn, s), SM: (g, sm), SP: (g, sp)}
    nn_to = (lax.rem(g + 2 + (G - 4) * odd, G), s)
    back = {FAR: FAR, NEAR: NEAR, SM: SP, SP: SM}
    nrow = marg.shape[1] // LANES
    erow = res.shape[0]
    stencil = sidx.shape[0]
    vrow = 4 * nrow
    sent = 2 * vrow
    tiles = [slice(i * 8, i * 8 + 8) for i in range(sq.shape[0] // 8)]

    barrier = pltpu.get_barrier_semaphore()
    for o in (FAR, NEAR, SM, SP):
        pl.semaphore_signal(barrier, inc=1, device_id=peer[o], device_id_type=MESH)
    pairs = (
        (head_h, head, 0), (res_h, res, 4), (tan_h, tan, 5), (send_h, own_send, 1), (tail_h, tail, 2),
        (coef_h, coef, 3), (marg_h, marg, 6), (sidx_h, sidx, 7), (scale_h, scale, 8),
    )
    local = [pltpu.make_async_copy(src, dst, send_sem.at[i]) for src, dst, i in pairs]
    for c in local:
        c.start()

    def copy_to(src, dst, ssem, rsem, who):
        return pltpu.make_async_remote_copy(
            src_ref=src, dst_ref=dst, send_sem=send_sem.at[ssem], recv_sem=recv_sem.at[rsem],
            device_id=who, device_id_type=MESH,
        )

    def landed(dst, rsem):
        copy_to(dst, dst, 0, rsem, peer[SP]).wait_recv()

    def left(src, ssem):
        copy_to(src, src, ssem, 0, peer[SP]).wait_send()

    def part_rows(ref, o):
        return ref.at[pl.ds((o - 1) * sent, sent)]

    def send_part(o):
        copy_to(part_rows(psend, o), part_rows(got_p, back[o]), 0, 0 if o == FAR else 1, peer[o]).start()

    def send_list(o):
        copy_to(own_send, got_send.at[back[o] - 1], 1, 2, peer[o]).start()

    def slot_rows(rnd, slot):
        return tab.at[rnd, pl.ds(slot * vrow, vrow)]

    def group(rnd, slot):
        if slot == FAR:
            return 0
        if slot > SP:
            return 1
        return 2 if rnd % 2 == 0 or slot > NEAR else 1

    def table_sem(rnd, slot):
        return 5 + (0, 3, 5, 8)[rnd] + group(rnd, slot) - rnd % 2

    def send_table(rnd, who, slot):
        copy_to(slot_rows(rnd, OWN), slot_rows(rnd, slot), 4 + rnd, table_sem(rnd, slot), who).start()

    def table_here(rnd, first, count=1):
        landed(tab.at[rnd, pl.ds(first * vrow, count * vrow)], table_sem(rnd, first))

    riota = lax.broadcasted_iota(I32, (vrow, LANES), 0)
    kind = riota // nrow
    rpart = (riota - kind * nrow).astype(F32).astype(BF16)
    lane16 = lax.broadcasted_iota(I32, (16, LANES), 0).astype(F32).astype(BF16)
    one, zero = jnp.ones((), BF16), jnp.zeros((), BF16)

    def cols_of(t):
        return slice(t * LANES, (t + 1) * LANES)

    def wide(row, rows):
        return jnp.broadcast_to(row.astype(F32), (rows, LANES)).astype(BF16)

    def lanes_onehot(ref, cols, x):
        lane = wide(x & (LANES - 1), 16)
        for q in range(LANES // 16):
            mine = lane16 + jnp.full((), 16 * q, BF16)
            ref[q * 16 : q * 16 + 16, cols] = jnp.where(mine == lane, one, zero)

    def split(val):
        hi = val.astype(BF16)
        return hi, (val - hi.astype(F32)).astype(BF16)

    def terms(t, sign):
        r = res[t : t + 1, :]
        val = jnp.broadcast_to(r if sign > 0 else -r, (vrow, LANES))
        half = 0.5 * r
        for c in range(3):
            val = jnp.where(kind == c + 1, tan[c : c + 1, cols_of(t)] * half, val)
        return split(val)

    def scatter(ref, rows_of, bases, sign, make=None):
        n = len(bases)
        for t in range(erow):
            cols = cols_of(t)
            x = rows_of[t : t + 1, :]
            if make:
                lanes_onehot(onehot, cols, x)
            pieces = terms(t, sign)
            row = wide(x >> 7, vrow)
            for j, base in enumerate(bases):
                hit = row == rpart + base
                for p, v in enumerate(pieces):
                    at = (p * n + j) * vrow
                    ref[at : at + vrow, cols] = jnp.where(hit, v, zero)
        both = nt_dot(ref[...], onehot[...])
        return both[: n * vrow] + both[n * vrow :]

    def base_of(block):
        return (jnp.asarray(block, I32) * nrow).astype(F32).astype(BF16)

    far_block, near_block = 1 + 2 * odd, 3 - 2 * odd

    for c in local[:4]:
        c.wait()
    psend[0:sent] = scatter(spread_f, head, [base_of(far_block), base_of(far_block + 1)], 1, make=True)

    def first_sends():
        pl.semaphore_wait(barrier, 4)
        send_part(FAR)
        for o in (FAR, NEAR, SM, SP):
            send_list(o)

    pl.when(g != 0)(first_sends)
    rest = scatter(
        spread_r, head,
        [base_of(b) for b in (near_block, near_block + 1, 5, 6, 7, 8, 0)], 1,
    )
    psend[sent:] = rest[: 3 * sent]
    own_sum = rest[3 * sent :]
    pl.when(g == 0)(first_sends)
    for o in (NEAR, SM, SP):
        send_part(o)
    for c in local[4:]:
        c.wait()

    if cf.shape[1] > stencil * nrow:
        cf[...] = jnp.zeros_like(cf)
        sq[...] = jnp.zeros_like(sq)
    for k in range(4):
        for r in range(nrow):
            cols = cols_of(r)
            c = coef[:, k, cols].astype(F32)
            d = (1.0 + marg[k : k + 1, cols]) * jnp.sum(jnp.abs(c), axis=0, keepdims=True)
            inv = 1.0 / d
            diag[k * nrow + r : k * nrow + r + 1, :] = inv
            cf[k, pl.ds(r, stencil, stride=nrow), :] = c * inv
    copy_to(cf, gcf, 2, 3, peer[FAR]).start()

    for t in range(erow):
        lanes_onehot(onehot, cols_of(t), tail[t : t + 1, :])
    own_sum = own_sum + scatter(spread_o, tail, [base_of(0)], -1)

    a_of = (odd, even)
    lists = tuple((f, b, r) for f in range(2) for b in range(2) for r in range(nrow))

    def own_list(f, b, r):
        return own_send[a_of[f], b : b + 1, cols_of(r)]

    for n, fbr in enumerate(lists):
        lanes_onehot(onehot3, cols_of(n), own_list(*fbr))
    for c in range(3):
        for t in range(erow):
            tan2[c * erow + t : c * erow + t + 1, :] = tan[c : c + 1, cols_of(t)]
    for r in range(nrow):
        sq[pl.ds(r, stencil, stride=nrow), :] = sidx[:, cols_of(r)]

    def place(ref, at, f, b, r):
        hit = wide(own_list(f, b, r) >> 7, vrow) == rpart
        base = b * vrow + r + at
        val = jnp.broadcast_to(ref[base : base + 1, :], (vrow, LANES))
        for k in range(1, 4):
            row = base + k * nrow
            val = jnp.where(kind == k, ref[row : row + 1, :], val)
        return [jnp.where(hit, v, zero) for v in split(val)]

    landed(got_p.at[pl.ds(sent, 3 * sent)], 1)
    for f in range(2):
        for b in range(2):
            first = pl.multiple_of((2 + b) * sent + a_of[f] * vrow, vrow)
            val = got_p[pl.ds(first, vrow), :]
            if f:
                val = val + got_p[sent + b * vrow : sent + (b + 1) * vrow, :]
            at = (f * 2 + b) * vrow
            tsum[at : at + vrow, :] = val
    for n, (f, b, r) in enumerate(lists):
        for p, v in enumerate(place(tsum, f * sent, f, b, r)):
            spread3[p * vrow : (p + 1) * vrow, cols_of(n)] = v
    got = nt_dot(spread3[...], onehot3[...])
    own_sum = own_sum + (got[:vrow] + got[vrow:])

    landed(part_rows(got_p, FAR), 0)
    half = len(lists) // 2
    for n, (f, b, r) in enumerate(lists[:half]):
        for p, v in enumerate(place(got_p, 0, f, b, r)):
            spread3[p * vrow : (p + 1) * vrow, cols_of(n)] = v
    got = nt_dot(spread3[:, : half * LANES], onehot3[:, : half * LANES])
    bsc[...] = (own_sum + (got[:vrow] + got[vrow:])) * diag[...]
    tab[0, :vrow, :] = bsc[...]

    def send_round(rnd, deep):
        if deep:
            send_table(rnd, peer[FAR], FAR)
            send_table(rnd, (gf, sp), FAR_SM)
            send_table(rnd, (gf, sm), FAR_SP)
            send_table(rnd, nn_to, FAR_NEAR)
        for o in (NEAR, SM, SP):
            send_table(rnd, peer[o], back[o])

    def compose(x):
        lane = x & (LANES - 1)
        row = x >> 7
        y = x
        for o in (FAR, NEAR, SM, SP):
            block = {FAR: far_block, NEAR: near_block, SM: 5, SP: 7}[o]
            for h in range(2):
                a, b = {FAR: (even, h), NEAR: (odd, h), SM: (h, 1), SP: (h, 0)}[o]
                for r in range(nrow):
                    line = got_send[o - 1, a, b : b + 1, cols_of(r)]
                    line = jnp.broadcast_to(line + o * nrow * LANES, x.shape)
                    y = jnp.where(row == (block + h) * nrow + r, lane_gather(line, lane), y)
        return y

    def compose_all():
        landed(got_send, 2)
        for w in tiles:
            sq[w, :] = compose(sq[w, :])
        copy_to(sq, gq, 3, 4, peer[FAR]).start()

    def compose_heads():
        for i in range(erow // 8):
            y = compose(head[i * 8 : i * 8 + 8, :])
            hq[i * 8 : i * 8 + 8, :] = y >> 7
            hl[i * 8 : i * 8 + 8, :] = y & (LANES - 1)

    def add_rows(rnd, slot, part, rows, lanes, accs):
        for i in range(len(rows)):
            for r in range(nrow):
                hit = rows[i] == part * nrow + r
                for k in range(4):
                    at = slot * vrow + k * nrow + r
                    line = jnp.broadcast_to(tab[rnd, at : at + 1, :], rows[i].shape)
                    v = lane_gather(line, lanes[i])
                    accs[i][k] = v if accs[i][k] is None else jnp.where(hit, v, accs[i][k])

    sub8 = lax.broadcasted_iota(I32, (8, LANES), 0)

    def sweep(rnd, index, factor, slots, start, out_slot, order, wait):
        where = [index[w, :] for w in tiles]
        rows = [y >> 7 for y in where]
        lanes = [y & (LANES - 1) for y in where]
        accs = [[None] * 4 for _ in tiles]
        for part in order:
            if part in wait:
                table_here(rnd, *wait[part])
            add_rows(rnd, slots[part], part, rows, lanes, accs)
        totals = []
        for k in range(4):
            total = None
            for w, acc in zip(tiles, accs):
                v = acc[k] * factor[k, w, :]
                total = v if total is None else total + v
            step = nrow
            while step < 8:
                total = total + pltpu.roll(total, step, axis=0)
                step *= 2
            totals.append(total)
        for at in range(0, vrow, 8):
            total = totals[at // nrow]
            for m in range(1, 8 // nrow):
                total = jnp.where(sub8 >= m * nrow, totals[at // nrow + m], total)
            to = out_slot * vrow + at
            tab[rnd + 1, to : to + 8, :] = start(at) - total

    def own_start(at):
        return bsc[at : at + 8, :]

    def ghost_start(at):
        return tab[0, FAR * vrow + at : FAR * vrow + at + 8, :]

    own_slots = (OWN, FAR, NEAR, SM, SP)
    for rnd in range(SWEEPS):
        deep = rnd % 2 == 0
        send_round(rnd, deep)
        if rnd == 0:
            compose_all()
        elif rnd == 1:
            compose_heads()
        if deep:
            sweep(
                rnd, sq, cf, own_slots, own_start, OWN,
                (OWN, SP, SM, NEAR, FAR), {SP: (NEAR, 3), FAR: (FAR, 1)},
            )
        else:
            table_here(rnd - 1, FAR_NEAR, 3)
            if rnd == 1:
                landed(gcf, 3)
                landed(gq, 4)
            sweep(rnd - 1, gq, gcf, GHOST_SLOT, ghost_start, FAR, (FAR, OWN, NEAR, SM, SP), {})
            if rnd < SWEEPS - 1:
                sweep(
                    rnd, sq, cf, own_slots, own_start, OWN,
                    (OWN, FAR, SP, SM, NEAR), {SP: (SM, 2), NEAR: (NEAR, 1)},
                )

    last = SWEEPS - 1
    where = [slice(i * 8, i * 8 + 8) for i in range(erow // 8)]
    tails = [tail[w, :] for w in where]
    tacc = [[None] * 4 for _ in where]
    add_rows(last, OWN, OWN, [t >> 7 for t in tails], [t & (LANES - 1) for t in tails], tacc)
    rows = [hq[w, :] for w in where]
    lanes = [hl[w, :] for w in where]
    hacc = [[None] * 4 for _ in where]
    for part in (OWN, FAR, SP, SM, NEAR):
        if part == SP:
            table_here(last, SM, 2)
        elif part == NEAR:
            table_here(last, NEAR)
        add_rows(last, part, part, rows, lanes, hacc)
    for i, w in enumerate(where):
        mixed = None
        for c in range(3):
            v = tan2[c * erow + i * 8 : c * erow + i * 8 + 8, :] * (tacc[i][c + 1] + hacc[i][c + 1])
            mixed = v if mixed is None else mixed + v
        out_ref[w, :] = scale[w, :] * res[w, :] + ((hacc[i][0] - tacc[i][0]) + 0.5 * mixed)

    left(psend, 0)
    left(got_send, 1)
    left(cf, 2)
    left(sq, 3)
    for rnd in range(SWEEPS):
        left(tab.at[rnd, pl.ds(0, (7 if rnd % 2 == 0 else 3) * vrow)], 4 + rnd)


def body(
    residual, edge_scale, tangent, edge_tail, edge_head,
    stencil_index, stencil_coef, diag_margin, send_index,
):
    edges = residual.shape[0]
    erow = edges // LANES
    nodes = diag_margin.shape[1]
    nrow = nodes // LANES
    vrow = 4 * nrow
    stencil = stencil_index.shape[0]
    qrow = -(-stencil * nrow // 8) * 8
    assert send_index.shape == (2, 2, nodes) and lax.axis_size("grp") % 2 == 0
    coef = jnp.transpose(stencil_coef, (1, 0, 2))
    square = lambda x: x.reshape(erow, LANES)
    anyspace = pl.BlockSpec(memory_space=pl.ANY)
    vm = pltpu.VMEM
    dma = pltpu.SemaphoreType.DMA
    out = pl.pallas_call(
        kernel,
        out_shape=vm((erow, LANES), F32),
        in_specs=[anyspace] * 9,
        out_specs=pl.BlockSpec(memory_space=vm),
        scratch_shapes=[
            vm((erow, LANES), F32),
            vm(tangent.shape, F32),
            vm((erow, LANES), I32),
            vm((erow, LANES), I32),
            vm(stencil_index.shape, I32),
            vm(coef.shape, BF16),
            vm(diag_margin.shape, F32),
            vm(send_index.shape, I32),
            vm((erow, LANES), F32),
            vm((4,) + send_index.shape, I32),
            vm((8 * vrow, LANES), F32),
            vm((8 * vrow, LANES), F32),
            vm((SWEEPS, SLOTS * vrow, LANES), F32),
            vm((LANES, edges), BF16),
            vm((2 * vrow, edges), BF16),
            vm((4 * vrow, edges), BF16),
            vm((14 * vrow, edges), BF16),
            vm((LANES, 4 * nodes), BF16),
            vm((2 * vrow, 4 * nodes), BF16),
            vm((4 * vrow, LANES), F32),
            vm((4, qrow, LANES), F32),
            vm((4, qrow, LANES), F32),
            vm((vrow, LANES), F32),
            vm((vrow, LANES), F32),
            vm((erow, LANES), I32),
            vm((erow, LANES), I32),
            vm((qrow, LANES), I32),
            vm((qrow, LANES), I32),
            vm((3 * erow, LANES), F32),
            dma((9,)),
            dma((15,)),
        ],
        compiler_params=pltpu.CompilerParams(collective_id=0, has_side_effects=True),
    )(
        square(residual), tangent, square(edge_tail), square(edge_head),
        stencil_index, coef, diag_margin, send_index, square(edge_scale),
    )
    return out.reshape(edges)


def solution(mesh):
    return jax.shard_map(
        body,
        mesh=mesh,
        in_specs=(
            P(("grp", "sub")),
            P(("grp", "sub")),
            P(None, ("grp", "sub")),
            P(("grp", "sub")),
            P(("grp", "sub")),
            P(None, ("grp", "sub")),
            P(None, None, ("grp", "sub")),
            P(None, ("grp", "sub")),
            P("grp", "sub", None),
        ),
        out_specs=P(("grp", "sub")),
        check_vma=False,
    )
```

```python
import jax
import jax.numpy as jnp
from jax import lax
from jax.experimental import pallas as pl
from jax.experimental.pallas import tpu as pltpu
from jax.sharding import PartitionSpec as P

SWEEPS = 4
LANES = 128
SLOTS = 8
MESH = pl.DeviceIdType.MESH
DNUMS = lax.GatherDimensionNumbers(
    offset_dims=(),
    collapsed_slice_dims=(1,),
    start_index_map=(1,),
    operand_batching_dims=(0,),
    start_indices_batching_dims=(0,),
)
F32 = jnp.float32
BF16 = jnp.bfloat16
I32 = jnp.int32

OWN, FAR, NEAR, SM, SP = range(5)
FAR_NEAR, FAR_SM, FAR_SP = 5, 6, 7
GHOST_SLOT = (FAR, OWN, FAR_NEAR, FAR_SM, FAR_SP)


def lane_gather(table, lane):
    return lax.gather(
        table,
        lane[..., None],
        DNUMS,
        slice_sizes=(1, 1),
        mode=lax.GatherScatterMode.PROMISE_IN_BOUNDS,
    )


def nt_dot(a, b):
    return lax.dot_general(a, b, (((1,), (1,)), ((), ())), preferred_element_type=F32)


def kernel(
    res_h, tan_h, tail_h, head_h, sidx_h, coef_h, marg_h, send_h, scale_h,
    out_ref,
    res, tan, tail, head, sidx, coef, marg, own_send, scale,
    got_send, psend, got_p, tab, onehot, spread_o, spread_f, spread_r, onehot3, spread3, tsum,
    cf, gcf, bsc, diag, hq, hl, sq, gq, tan2,
    send_sem, recv_sem,
):
    G, S = lax.axis_size("grp"), lax.axis_size("sub")
    g, s = lax.axis_index("grp"), lax.axis_index("sub")
    odd = lax.rem(g, 2)
    even = 1 - odd
    gf, gn = lax.rem(g + G - 1 + 2 * odd, G), lax.rem(g + 1 + (G - 2) * odd, G)
    sm, sp = lax.rem(s + S - 1, S), lax.rem(s + 1, S)
    peer = {FAR: (gf, s), NEAR: (gn, s), SM: (g, sm), SP: (g, sp)}
    nn_to = (lax.rem(g + 2 + (G - 4) * odd, G), s)
    back = {FAR: FAR, NEAR: NEAR, SM: SP, SP: SM}
    nrow = marg.shape[1] // LANES
    erow = res.shape[0]
    stencil = sidx.shape[0]
    vrow = 4 * nrow
    sent = 2 * vrow
    tiles = [slice(i * 8, i * 8 + 8) for i in range(sq.shape[0] // 8)]

    barrier = pltpu.get_barrier_semaphore()
    for o in (FAR, NEAR, SM, SP):
        pl.semaphore_signal(barrier, inc=1, device_id=peer[o], device_id_type=MESH)
    pairs = (
        (head_h, head, 0), (res_h, res, 4), (tan_h, tan, 5), (send_h, own_send, 1), (tail_h, tail, 2),
        (coef_h, coef, 3), (marg_h, marg, 6), (sidx_h, sidx, 7), (scale_h, scale, 8),
    )
    local = [pltpu.make_async_copy(src, dst, send_sem.at[i]) for src, dst, i in pairs]
    for c in local:
        c.start()

    def copy_to(src, dst, ssem, rsem, who):
        return pltpu.make_async_remote_copy(
            src_ref=src, dst_ref=dst, send_sem=send_sem.at[ssem], recv_sem=recv_sem.at[rsem],
            device_id=who, device_id_type=MESH,
        )

    def landed(dst, rsem):
        copy_to(dst, dst, 0, rsem, peer[SP]).wait_recv()

    def left(src, ssem):
        copy_to(src, src, ssem, 0, peer[SP]).wait_send()

    def part_rows(ref, o):
        return ref.at[pl.ds((o - 1) * sent, sent)]

    def send_part(o):
        far = o == FAR
        copy_to(part_rows(psend, o), part_rows(got_p, back[o]), 9 if far else 0, 0 if far else 1, peer[o]).start()

    def send_list(o):
        copy_to(own_send, got_send.at[back[o] - 1], 1, 2, peer[o]).start()

    def slot_rows(rnd, slot):
        return tab.at[rnd, pl.ds(slot * vrow, vrow)]

    def table_sem(rnd, slot):
        own = slot + 3 if rnd % 2 else min(slot, FAR_NEAR) - 1 if isinstance(slot, int) else slot - 1
        return 5 + SLOTS * (rnd // 2) + own

    def send_table(rnd, who, slot):
        copy_to(slot_rows(rnd, OWN), slot_rows(rnd, slot), 4 + rnd, table_sem(rnd, slot), who).start()

    def table_here(rnd, first, count=1):
        landed(tab.at[rnd, pl.ds(first * vrow, count * vrow)], table_sem(rnd, first))

    riota = lax.broadcasted_iota(I32, (vrow, LANES), 0)
    kind = riota // nrow
    rpart = (riota - kind * nrow).astype(F32).astype(BF16)
    lane16 = lax.broadcasted_iota(I32, (16, LANES), 0).astype(F32).astype(BF16)
    one, zero = jnp.ones((), BF16), jnp.zeros((), BF16)

    def cols_of(t):
        return slice(t * LANES, (t + 1) * LANES)

    def wide(row, rows):
        return jnp.broadcast_to(row.astype(F32), (rows, LANES)).astype(BF16)

    def lanes_onehot(ref, cols, x):
        lane = wide(x & (LANES - 1), 16)
        for q in range(LANES // 16):
            mine = lane16 + jnp.full((), 16 * q, BF16)
            ref[q * 16 : q * 16 + 16, cols] = jnp.where(mine == lane, one, zero)

    def split(val):
        hi = val.astype(BF16)
        return hi, (val - hi.astype(F32)).astype(BF16)

    def terms(t, sign):
        r = res[t : t + 1, :]
        val = jnp.broadcast_to(r if sign > 0 else -r, (vrow, LANES))
        half = 0.5 * r
        for c in range(3):
            val = jnp.where(kind == c + 1, tan[c : c + 1, cols_of(t)] * half, val)
        return split(val)

    def scatter(ref, rows_of, bases, sign, make=None):
        n = len(bases)
        for t in range(erow):
            cols = cols_of(t)
            x = rows_of[t : t + 1, :]
            if make:
                lanes_onehot(onehot, cols, x)
            pieces = terms(t, sign)
            row = wide(x >> 7, vrow)
            for j, base in enumerate(bases):
                hit = row == rpart + base
                for p, v in enumerate(pieces):
                    at = (p * n + j) * vrow
                    ref[at : at + vrow, cols] = jnp.where(hit, v, zero)
        both = nt_dot(ref[...], onehot[...])
        return both[: n * vrow] + both[n * vrow :]

    def base_of(block):
        return (jnp.asarray(block, I32) * nrow).astype(F32).astype(BF16)

    far_block, near_block = 1 + 2 * odd, 3 - 2 * odd

    for c in local[:4]:
        c.wait()
    psend[0:sent] = scatter(spread_f, head, [base_of(far_block), base_of(far_block + 1)], 1, make=True)

    def first_sends():
        pl.semaphore_wait(barrier, 4)
        send_part(FAR)
        for o in (FAR, NEAR, SM, SP):
            send_list(o)

    pl.when(g != 0)(first_sends)
    rest = scatter(
        spread_r, head,
        [base_of(b) for b in (near_block, near_block + 1, 5, 6, 7, 8, 0)], 1,
    )
    psend[sent:] = rest[: 3 * sent]
    own_sum = rest[3 * sent :]
    pl.when(g == 0)(first_sends)
    for o in (NEAR, SM, SP):
        send_part(o)
    for c in local[4:]:
        c.wait()

    if cf.shape[1] > stencil * nrow:
        cf[...] = jnp.zeros_like(cf)
        sq[...] = jnp.zeros_like(sq)
    for k in range(4):
        for r in range(nrow):
            cols = cols_of(r)
            c = coef[:, k, cols].astype(F32)
            d = (1.0 + marg[k : k + 1, cols]) * jnp.sum(jnp.abs(c), axis=0, keepdims=True)
            inv = 1.0 / d
            diag[k * nrow + r : k * nrow + r + 1, :] = inv
            cf[k, pl.ds(r, stencil, stride=nrow), :] = c * inv

    for t in range(erow):
        lanes_onehot(onehot, cols_of(t), tail[t : t + 1, :])
    own_sum = own_sum + scatter(spread_o, tail, [base_of(0)], -1)

    a_of = (odd, even)
    lists = tuple((f, b, r) for f in range(2) for b in range(2) for r in range(nrow))

    def own_list(f, b, r):
        return own_send[a_of[f], b : b + 1, cols_of(r)]

    for n, fbr in enumerate(lists):
        lanes_onehot(onehot3, cols_of(n), own_list(*fbr))
    for c in range(3):
        for t in range(erow):
            tan2[c * erow + t : c * erow + t + 1, :] = tan[c : c + 1, cols_of(t)]
    for r in range(nrow):
        sq[pl.ds(r, stencil, stride=nrow), :] = sidx[:, cols_of(r)]

    def place(ref, at, f, b, r):
        hit = wide(own_list(f, b, r) >> 7, vrow) == rpart
        base = b * vrow + r + at
        val = jnp.broadcast_to(ref[base : base + 1, :], (vrow, LANES))
        for k in range(1, 4):
            row = base + k * nrow
            val = jnp.where(kind == k, ref[row : row + 1, :], val)
        return [jnp.where(hit, v, zero) for v in split(val)]

    parts_left = lambda: left(psend.at[pl.ds(sent, 3 * sent)], 0)
    pl.when(g != 0)(parts_left)
    copy_to(cf, gcf, 2, 3, peer[FAR]).start()
    landed(got_p.at[pl.ds(sent, 3 * sent)], 1)
    for f in range(2):
        for b in range(2):
            first = pl.multiple_of((2 + b) * sent + a_of[f] * vrow, vrow)
            val = got_p[pl.ds(first, vrow), :]
            if f:
                val = val + got_p[sent + b * vrow : sent + (b + 1) * vrow, :]
            at = (f * 2 + b) * vrow
            tsum[at : at + vrow, :] = val
    for n, (f, b, r) in enumerate(lists):
        for p, v in enumerate(place(tsum, f * sent, f, b, r)):
            spread3[p * vrow : (p + 1) * vrow, cols_of(n)] = v
    got = nt_dot(spread3[...], onehot3[...])
    own_sum = own_sum + (got[:vrow] + got[vrow:])

    landed(part_rows(got_p, FAR), 0)
    half = len(lists) // 2
    for n, (f, b, r) in enumerate(lists[:half]):
        for p, v in enumerate(place(got_p, 0, f, b, r)):
            spread3[p * vrow : (p + 1) * vrow, cols_of(n)] = v
    got = nt_dot(spread3[:, : half * LANES], onehot3[:, : half * LANES])
    bsc[...] = (own_sum + (got[:vrow] + got[vrow:])) * diag[...]
    tab[0, :vrow, :] = bsc[...]

    def send_round(rnd, deep):
        if deep:
            send_table(rnd, peer[FAR], FAR)
        for o in (NEAR, SM, SP):
            send_table(rnd, peer[o], back[o])
        if deep:
            send_table(rnd, (gf, sp), FAR_SM)
            send_table(rnd, (gf, sm), FAR_SP)
            send_table(rnd, nn_to, FAR_NEAR)

    def compose(x):
        lane = x & (LANES - 1)
        row = x >> 7
        y = x
        for o in (FAR, NEAR, SM, SP):
            block = {FAR: far_block, NEAR: near_block, SM: 5, SP: 7}[o]
            for h in range(2):
                a, b = {FAR: (even, h), NEAR: (odd, h), SM: (h, 1), SP: (h, 0)}[o]
                for r in range(nrow):
                    line = got_send[o - 1, a, b : b + 1, cols_of(r)]
                    line = jnp.broadcast_to(line + o * nrow * LANES, x.shape)
                    y = jnp.where(row == (block + h) * nrow + r, lane_gather(line, lane), y)
        return y

    def compose_all():
        landed(got_send, 2)
        for w in tiles:
            sq[w, :] = compose(sq[w, :])
        copy_to(sq, gq, 3, 4, peer[FAR]).start()

    def compose_heads():
        for i in range(erow // 8):
            y = compose(head[i * 8 : i * 8 + 8, :])
            hq[i * 8 : i * 8 + 8, :] = y >> 7
            hl[i * 8 : i * 8 + 8, :] = y & (LANES - 1)

    def add_rows(rnd, slot, part, rows, lanes, accs):
        for i in range(len(rows)):
            for r in range(nrow):
                hit = rows[i] == part * nrow + r
                for k in range(4):
                    at = slot * vrow + k * nrow + r
                    line = jnp.broadcast_to(tab[rnd, pl.ds(at, 1), :], rows[i].shape)
                    v = lane_gather(line, lanes[i])
                    accs[i][k] = v if accs[i][k] is None else jnp.where(hit, v, accs[i][k])

    sub8 = lax.broadcasted_iota(I32, (8, LANES), 0)

    def open_sweep(rnd, index):
        where = [index[w, :] for w in tiles]
        rows = [y >> 7 for y in where]
        lanes = [y & (LANES - 1) for y in where]
        accs = [[None] * 4 for _ in tiles]

        def add(part, slot=None):
            add_rows(rnd, part if slot is None else slot, part, rows, lanes, accs)

        return add, accs

    def close_sweep(rnd, accs, factor, start, out_slot):
        totals = []
        for k in range(4):
            total = None
            for w, acc in zip(tiles, accs):
                v = acc[k] * factor[k, w, :]
                total = v if total is None else total + v
            step = nrow
            while step < 8:
                total = total + pltpu.roll(total, step, axis=0)
                step *= 2
            totals.append(total)
        for at in range(0, vrow, 8):
            total = totals[at // nrow]
            for m in range(1, 8 // nrow):
                total = jnp.where(sub8 >= m * nrow, totals[at // nrow + m], total)
            to = out_slot * vrow + at
            tab[rnd + 1, to : to + 8, :] = start(at) - total

    def own_start(at):
        return bsc[at : at + 8, :]

    def ghost_start(at):
        return tab[0, FAR * vrow + at : FAR * vrow + at + 8, :]

    s_odd = lax.rem(s, 2)
    arrivals = (SP - s_odd, SM - s_odd, NEAR + 2 * s_odd)

    for rnd in range(0, SWEEPS, 2):
        send_round(rnd, True)
        if rnd == 0:
            compose_all()
            compose_heads()
        add, accs = open_sweep(rnd, sq)
        add(OWN)
        for part in arrivals + (FAR,):
            table_here(rnd, part)
            add(part)
        close_sweep(rnd, accs, cf, own_start, OWN)
        send_round(rnd + 1, False)

        final = rnd + 2 == SWEEPS
        if final:
            where = [slice(i * 8, i * 8 + 8) for i in range(erow // 8)]
            tails = [tail[w, :] for w in where]
            tacc = [[None] * 4 for _ in where]
            add_rows(rnd + 1, OWN, OWN, [t >> 7 for t in tails], [t & (LANES - 1) for t in tails], tacc)
            rows = [hq[w, :] for w in where]
            lanes = [hl[w, :] for w in where]
            hacc = [[None] * 4 for _ in where]

            def add(part):
                add_rows(rnd + 1, part, part, rows, lanes, hacc)
        else:
            add, accs = open_sweep(rnd + 1, sq)
        add(OWN)
        if rnd == 0:
            landed(gq, 4)
        ghost_add, ghost_accs = open_sweep(rnd, gq)
        ghost_add(OWN, FAR)
        ghost_add(FAR, OWN)
        table_here(rnd, FAR_NEAR, 3)
        for part in (NEAR, SM, SP):
            ghost_add(part, GHOST_SLOT[part])
        if rnd == 0:
            landed(gcf, 3)
        close_sweep(rnd, ghost_accs, gcf, ghost_start, FAR)
        add(FAR)
        for part in arrivals:
            table_here(rnd + 1, part)
            add(part)
        if not final:
            close_sweep(rnd + 1, accs, cf, own_start, OWN)

    for i, w in enumerate(where):
        mixed = None
        for c in range(3):
            v = tan2[c * erow + i * 8 : c * erow + i * 8 + 8, :] * (tacc[i][c + 1] + hacc[i][c + 1])
            mixed = v if mixed is None else mixed + v
        out_ref[w, :] = scale[w, :] * res[w, :] + ((hacc[i][0] - tacc[i][0]) + 0.5 * mixed)

    pl.when(g == 0)(parts_left)
    left(part_rows(psend, FAR), 9)
    left(got_send, 1)
    left(cf, 2)
    left(sq, 3)
    for rnd in range(SWEEPS):
        left(tab.at[rnd, pl.ds(0, (7 if rnd % 2 == 0 else 3) * vrow)], 4 + rnd)


def body(
    residual, edge_scale, tangent, edge_tail, edge_head,
    stencil_index, stencil_coef, diag_margin, send_index,
):
    edges = residual.shape[0]
    erow = edges // LANES
    nodes = diag_margin.shape[1]
    nrow = nodes // LANES
    vrow = 4 * nrow
    stencil = stencil_index.shape[0]
    qrow = -(-stencil * nrow // 8) * 8
    assert send_index.shape == (2, 2, nodes) and lax.axis_size("grp") % 2 == 0
    coef = jnp.transpose(stencil_coef, (1, 0, 2))
    square = lambda x: x.reshape(erow, LANES)
    anyspace = pl.BlockSpec(memory_space=pl.ANY)
    vm = pltpu.VMEM
    dma = pltpu.SemaphoreType.DMA
    out = pl.pallas_call(
        kernel,
        out_shape=vm((erow, LANES), F32),
        in_specs=[anyspace] * 9,
        out_specs=pl.BlockSpec(memory_space=vm),
        scratch_shapes=[
            vm((erow, LANES), F32),
            vm(tangent.shape, F32),
            vm((erow, LANES), I32),
            vm((erow, LANES), I32),
            vm(stencil_index.shape, I32),
            vm(coef.shape, BF16),
            vm(diag_margin.shape, F32),
            vm(send_index.shape, I32),
            vm((erow, LANES), F32),
            vm((4,) + send_index.shape, I32),
            vm((8 * vrow, LANES), F32),
            vm((8 * vrow, LANES), F32),
            vm((SWEEPS, SLOTS * vrow, LANES), F32),
            vm((LANES, edges), BF16),
            vm((2 * vrow, edges), BF16),
            vm((4 * vrow, edges), BF16),
            vm((14 * vrow, edges), BF16),
            vm((LANES, 4 * nodes), BF16),
            vm((2 * vrow, 4 * nodes), BF16),
            vm((4 * vrow, LANES), F32),
            vm((4, qrow, LANES), F32),
            vm((4, qrow, LANES), F32),
            vm((vrow, LANES), F32),
            vm((vrow, LANES), F32),
            vm((erow, LANES), I32),
            vm((erow, LANES), I32),
            vm((qrow, LANES), I32),
            vm((qrow, LANES), I32),
            vm((3 * erow, LANES), F32),
            dma((10,)),
            dma((5 + SLOTS * (SWEEPS // 2),)),
        ],
        compiler_params=pltpu.CompilerParams(collective_id=0, has_side_effects=True),
    )(
        square(residual), tangent, square(edge_tail), square(edge_head),
        stencil_index, coef, diag_margin, send_index, square(edge_scale),
    )
    return out.reshape(edges)


def solution(mesh):
    return jax.shard_map(
        body,
        mesh=mesh,
        in_specs=(
            P(("grp", "sub")),
            P(("grp", "sub")),
            P(None, ("grp", "sub")),
            P(("grp", "sub")),
            P(("grp", "sub")),
            P(None, ("grp", "sub")),
            P(None, None, ("grp", "sub")),
            P(None, ("grp", "sub")),
            P("grp", "sub", None),
        ),
        out_specs=P(("grp", "sub")),
        check_vma=False,
    )
```

```python
import jax
import jax.numpy as jnp
from jax import lax
from jax.experimental import pallas as pl
from jax.experimental.pallas import tpu as pltpu
from jax.sharding import PartitionSpec as P

SWEEPS = 4
LANES = 128
SLOTS = 8
MESH = pl.DeviceIdType.MESH
DNUMS = lax.GatherDimensionNumbers(
    offset_dims=(),
    collapsed_slice_dims=(1,),
    start_index_map=(1,),
    operand_batching_dims=(0,),
    start_indices_batching_dims=(0,),
)
F32 = jnp.float32
BF16 = jnp.bfloat16
I32 = jnp.int32

OWN, FAR, NEAR, SM, SP = range(5)
FAR_NEAR, FAR_SM, FAR_SP = 5, 6, 7
GHOST_SLOT = (FAR, OWN, FAR_NEAR, FAR_SM, FAR_SP)


def lane_gather(table, lane):
    return lax.gather(
        table,
        lane[..., None],
        DNUMS,
        slice_sizes=(1, 1),
        mode=lax.GatherScatterMode.PROMISE_IN_BOUNDS,
    )


def nt_dot(a, b):
    return lax.dot_general(a, b, (((1,), (1,)), ((), ())), preferred_element_type=F32)


def kernel(
    res_h, tan_h, tail_h, head_h, sidx_h, coef_h, marg_h, send_h, scale_h,
    out_ref,
    res, tan, tail, head, sidx, coef, marg, own_send, scale,
    got_send, psend, got_p, tab, onehot, spread_o, spread_f, spread_r, onehot3, spread3, tsum,
    cf, gcf, bsc, diag, hq, hl, sq, gq, tan2,
    send_sem, recv_sem,
):
    G, S = lax.axis_size("grp"), lax.axis_size("sub")
    g, s = lax.axis_index("grp"), lax.axis_index("sub")
    odd = lax.rem(g, 2)
    even = 1 - odd
    gf, gn = lax.rem(g + G - 1 + 2 * odd, G), lax.rem(g + 1 + (G - 2) * odd, G)
    sm, sp = lax.rem(s + S - 1, S), lax.rem(s + 1, S)
    peer = {FAR: (gf, s), NEAR: (gn, s), SM: (g, sm), SP: (g, sp)}
    nn_to = (lax.rem(g + 2 + (G - 4) * odd, G), s)
    seam = (g == 0) | (g == G - 1)
    plain = (g != 0) & (g != G - 1)
    feeds = (g == 1) | (g == G - 2)
    inner = plain & (g != 1) & (g != G - 2)
    back = {FAR: FAR, NEAR: NEAR, SM: SP, SP: SM}
    nrow = marg.shape[1] // LANES
    erow = res.shape[0]
    stencil = sidx.shape[0]
    vrow = 4 * nrow
    sent = 2 * vrow
    tiles = [slice(i * 8, i * 8 + 8) for i in range(sq.shape[0] // 8)]

    barrier = pltpu.get_barrier_semaphore()
    for o in (FAR, NEAR, SM, SP):
        pl.semaphore_signal(barrier, inc=1, device_id=peer[o], device_id_type=MESH)
    pairs = (
        (head_h, head, 0), (res_h, res, 4), (tan_h, tan, 5), (send_h, own_send, 1), (tail_h, tail, 2),
        (coef_h, coef, 3), (marg_h, marg, 6), (sidx_h, sidx, 7), (scale_h, scale, 8),
    )
    local = [pltpu.make_async_copy(src, dst, send_sem.at[i]) for src, dst, i in pairs]
    for c in local:
        c.start()

    def copy_to(src, dst, ssem, rsem, who):
        return pltpu.make_async_remote_copy(
            src_ref=src, dst_ref=dst, send_sem=send_sem.at[ssem], recv_sem=recv_sem.at[rsem],
            device_id=who, device_id_type=MESH,
        )

    def landed(dst, rsem):
        copy_to(dst, dst, 0, rsem, peer[SP]).wait_recv()

    def left(src, ssem):
        copy_to(src, src, ssem, 0, peer[SP]).wait_send()

    def part_rows(ref, o):
        return ref.at[pl.ds((o - 1) * sent, sent)]

    def send_part(o):
        far = o == FAR
        copy_to(part_rows(psend, o), part_rows(got_p, back[o]), 9 if far else 0, 0 if far else 1, peer[o]).start()

    def send_list(o):
        copy_to(own_send, got_send.at[back[o] - 1], 1, 2, peer[o]).start()

    def slot_rows(rnd, slot):
        return tab.at[rnd, pl.ds(slot * vrow, vrow)]

    def table_sem(rnd, slot):
        slot = min(slot, FAR_NEAR) if isinstance(slot, int) else slot
        return 5 + 9 * (rnd // 2) + slot - 1 + FAR_NEAR * (rnd % 2)

    def send_table(rnd, who, slot):
        copy_to(slot_rows(rnd, OWN), slot_rows(rnd, slot), 4 + rnd, table_sem(rnd, slot), who).start()

    def table_here(rnd, first, count=1):
        landed(tab.at[rnd, pl.ds(first * vrow, count * vrow)], table_sem(rnd, first))

    riota = lax.broadcasted_iota(I32, (vrow, LANES), 0)
    kind = riota // nrow
    rpart = (riota - kind * nrow).astype(F32).astype(BF16)
    lane16 = lax.broadcasted_iota(I32, (16, LANES), 0).astype(F32).astype(BF16)
    one, zero = jnp.ones((), BF16), jnp.zeros((), BF16)

    def cols_of(t):
        return slice(t * LANES, (t + 1) * LANES)

    def wide(row, rows):
        return jnp.broadcast_to(row.astype(F32), (rows, LANES)).astype(BF16)

    def lanes_onehot(ref, cols, x):
        lane = wide(x & (LANES - 1), 16)
        for q in range(LANES // 16):
            mine = lane16 + jnp.full((), 16 * q, BF16)
            ref[q * 16 : q * 16 + 16, cols] = jnp.where(mine == lane, one, zero)

    def split(val):
        hi = val.astype(BF16)
        return hi, (val - hi.astype(F32)).astype(BF16)

    def terms(t, sign):
        r = res[t : t + 1, :]
        val = jnp.broadcast_to(r if sign > 0 else -r, (vrow, LANES))
        half = 0.5 * r
        for c in range(3):
            val = jnp.where(kind == c + 1, tan[c : c + 1, cols_of(t)] * half, val)
        return split(val)

    def scatter(ref, rows_of, bases, sign, make=None):
        n = len(bases)
        for t in range(erow):
            cols = cols_of(t)
            x = rows_of[t : t + 1, :]
            if make:
                lanes_onehot(onehot, cols, x)
            pieces = terms(t, sign)
            row = wide(x >> 7, vrow)
            for j, base in enumerate(bases):
                hit = row == rpart + base
                for p, v in enumerate(pieces):
                    at = (p * n + j) * vrow
                    ref[at : at + vrow, cols] = jnp.where(hit, v, zero)
        both = nt_dot(ref[...], onehot[...])
        return both[: n * vrow] + both[n * vrow :]

    def base_of(block):
        return (jnp.asarray(block, I32) * nrow).astype(F32).astype(BF16)

    far_block, near_block = 1 + 2 * odd, 3 - 2 * odd

    for c in local[:4]:
        c.wait()
    psend[0:sent] = scatter(spread_f, head, [base_of(far_block), base_of(far_block + 1)], 1, make=True)

    def first_sends():
        pl.semaphore_wait(barrier, 4)
        send_part(FAR)
        for o in (FAR, NEAR, SM, SP):
            send_list(o)

    pl.when(g != 0)(first_sends)
    rest = scatter(
        spread_r, head,
        [base_of(b) for b in (near_block, near_block + 1, 5, 6, 7, 8, 0)], 1,
    )
    psend[sent:] = rest[: 3 * sent]
    own_sum = rest[3 * sent :]
    pl.when(g == 0)(first_sends)
    for o in (NEAR, SM, SP):
        send_part(o)
    for c in local[4:]:
        c.wait()

    if cf.shape[1] > stencil * nrow:
        cf[...] = jnp.zeros_like(cf)
        sq[...] = jnp.zeros_like(sq)
    for k in range(4):
        for r in range(nrow):
            cols = cols_of(r)
            c = coef[:, k, cols].astype(F32)
            d = (1.0 + marg[k : k + 1, cols]) * jnp.sum(jnp.abs(c), axis=0, keepdims=True)
            inv = 1.0 / d
            diag[k * nrow + r : k * nrow + r + 1, :] = inv
            cf[k, pl.ds(r, stencil, stride=nrow), :] = c * inv

    for t in range(erow):
        lanes_onehot(onehot, cols_of(t), tail[t : t + 1, :])
    own_sum = own_sum + scatter(spread_o, tail, [base_of(0)], -1)

    a_of = (odd, even)
    lists = tuple((f, b, r) for f in range(2) for b in range(2) for r in range(nrow))

    def own_list(f, b, r):
        return own_send[a_of[f], b : b + 1, cols_of(r)]

    for n, fbr in enumerate(lists):
        lanes_onehot(onehot3, cols_of(n), own_list(*fbr))
    for c in range(3):
        for t in range(erow):
            tan2[c * erow + t : c * erow + t + 1, :] = tan[c : c + 1, cols_of(t)]
    for r in range(nrow):
        sq[pl.ds(r, stencil, stride=nrow), :] = sidx[:, cols_of(r)]

    def place(ref, at, f, b, r):
        hit = wide(own_list(f, b, r) >> 7, vrow) == rpart
        base = b * vrow + r + at
        val = jnp.broadcast_to(ref[base : base + 1, :], (vrow, LANES))
        for k in range(1, 4):
            row = base + k * nrow
            val = jnp.where(kind == k, ref[row : row + 1, :], val)
        return [jnp.where(hit, v, zero) for v in split(val)]

    parts_left = lambda: left(psend.at[pl.ds(sent, 3 * sent)], 0)
    pl.when(g == G - 1)(parts_left)

    @pl.when(seam)
    def _():
        copy_to(cf, gcf, 2, 3, peer[FAR]).start()

    landed(got_p.at[pl.ds(sent, 3 * sent)], 1)
    for f in range(2):
        for b in range(2):
            first = pl.multiple_of((2 + b) * sent + a_of[f] * vrow, vrow)
            val = got_p[pl.ds(first, vrow), :]
            if f:
                val = val + got_p[sent + b * vrow : sent + (b + 1) * vrow, :]
            at = (f * 2 + b) * vrow
            tsum[at : at + vrow, :] = val
    for n, (f, b, r) in enumerate(lists):
        for p, v in enumerate(place(tsum, f * sent, f, b, r)):
            spread3[p * vrow : (p + 1) * vrow, cols_of(n)] = v
    got = nt_dot(spread3[...], onehot3[...])
    own_sum = own_sum + (got[:vrow] + got[vrow:])

    landed(part_rows(got_p, FAR), 0)
    half = len(lists) // 2
    for n, (f, b, r) in enumerate(lists[:half]):
        for p, v in enumerate(place(got_p, 0, f, b, r)):
            spread3[p * vrow : (p + 1) * vrow, cols_of(n)] = v
    got = nt_dot(spread3[:, : half * LANES], onehot3[:, : half * LANES])
    bsc[...] = (own_sum + (got[:vrow] + got[vrow:])) * diag[...]
    tab[0, :vrow, :] = bsc[...]

    def send_round(rnd, deep):
        if deep:
            send_table(rnd, peer[FAR], FAR)
        for o in (NEAR, SM, SP):
            send_table(rnd, peer[o], back[o])
        if deep:
            @pl.when(seam)
            def _():
                send_table(rnd, (gf, sp), FAR_SM)
                send_table(rnd, (gf, sm), FAR_SP)

            @pl.when(feeds)
            def _():
                send_table(rnd, nn_to, FAR_NEAR)
        else:
            @pl.when(plain)
            def _():
                send_table(rnd, peer[FAR], FAR)

    def compose(x):
        lane = x & (LANES - 1)
        row = x >> 7
        y = x
        for o in (FAR, NEAR, SM, SP):
            block = {FAR: far_block, NEAR: near_block, SM: 5, SP: 7}[o]
            for h in range(2):
                a, b = {FAR: (even, h), NEAR: (odd, h), SM: (h, 1), SP: (h, 0)}[o]
                for r in range(nrow):
                    line = got_send[o - 1, a, b : b + 1, cols_of(r)]
                    line = jnp.broadcast_to(line + o * nrow * LANES, x.shape)
                    y = jnp.where(row == (block + h) * nrow + r, lane_gather(line, lane), y)
        return y

    def compose_all():
        landed(got_send, 2)
        for w in tiles:
            sq[w, :] = compose(sq[w, :])

        @pl.when(seam)
        def _():
            copy_to(sq, gq, 3, 4, peer[FAR]).start()

    def compose_heads():
        for i in range(erow // 8):
            y = compose(head[i * 8 : i * 8 + 8, :])
            hq[i * 8 : i * 8 + 8, :] = y >> 7
            hl[i * 8 : i * 8 + 8, :] = y & (LANES - 1)

    def add_rows(rnd, slot, part, rows, lanes, accs):
        for i in range(len(rows)):
            for r in range(nrow):
                hit = rows[i] == part * nrow + r
                for k in range(4):
                    at = slot * vrow + k * nrow + r
                    line = jnp.broadcast_to(tab[rnd, pl.ds(at, 1), :], rows[i].shape)
                    v = lane_gather(line, lanes[i])
                    accs[i][k] = v if accs[i][k] is None else jnp.where(hit, v, accs[i][k])

    sub8 = lax.broadcasted_iota(I32, (8, LANES), 0)

    def open_sweep(rnd, index):
        where = [index[w, :] for w in tiles]
        rows = [y >> 7 for y in where]
        lanes = [y & (LANES - 1) for y in where]
        accs = [[None] * 4 for _ in tiles]

        def add(part, slot=None):
            add_rows(rnd, part if slot is None else slot, part, rows, lanes, accs)

        return add, accs

    def close_sweep(rnd, accs, factor, start, out_slot):
        totals = []
        for k in range(4):
            total = None
            for w, acc in zip(tiles, accs):
                v = acc[k] * factor[k, w, :]
                total = v if total is None else total + v
            step = nrow
            while step < 8:
                total = total + pltpu.roll(total, step, axis=0)
                step *= 2
            totals.append(total)
        for at in range(0, vrow, 8):
            total = totals[at // nrow]
            for m in range(1, 8 // nrow):
                total = jnp.where(sub8 >= m * nrow, totals[at // nrow + m], total)
            to = out_slot * vrow + at
            tab[rnd + 1, to : to + 8, :] = start(at) - total

    def own_start(at):
        return bsc[at : at + 8, :]

    def ghost_start(at):
        return tab[0, FAR * vrow + at : FAR * vrow + at + 8, :]

    s_odd = lax.rem(s, 2)
    partner, across = SP - s_odd, SM + s_odd
    second, third = SM - s_odd, NEAR + 2 * s_odd

    def either(here, there):
        return [jnp.where(seam, a, b) for a, b in zip(here, there)]

    slow_order = (
        either((partner, second, third, FAR), (partner, across, FAR, NEAR)),
        either((partner, second, FAR, third), (partner, across, FAR, NEAR)),
    )
    fast_order = either((FAR, partner, second, third), (partner, across, FAR, NEAR))

    for rnd in range(0, SWEEPS, 2):
        send_round(rnd, True)
        if rnd == 0:
            compose_all()
            compose_heads()
        add, accs = open_sweep(rnd, sq)
        add(OWN)
        for part in slow_order[rnd // 2]:
            table_here(rnd, part)
            add(part)
        close_sweep(rnd, accs, cf, own_start, OWN)
        send_round(rnd + 1, False)

        final = rnd + 2 == SWEEPS
        if final:
            where = [slice(i * 8, i * 8 + 8) for i in range(erow // 8)]
            tails = [tail[w, :] for w in where]
            tacc = [[None] * 4 for _ in where]
            add_rows(rnd + 1, OWN, OWN, [t >> 7 for t in tails], [t & (LANES - 1) for t in tails], tacc)
            rows = [hq[w, :] for w in where]
            lanes = [hl[w, :] for w in where]
            hacc = [[None] * 4 for _ in where]

            def add(part):
                add_rows(rnd + 1, part, part, rows, lanes, hacc)
        else:
            add, accs = open_sweep(rnd + 1, sq)
        add(OWN)

        @pl.when(seam)
        def _():
            if rnd == 0:
                landed(gq, 4)
            ghost_add, ghost_accs = open_sweep(rnd, gq)
            ghost_add(OWN, FAR)
            ghost_add(FAR, OWN)
            table_here(rnd, FAR_NEAR, 3)
            for part in (NEAR, SM, SP):
                ghost_add(part, GHOST_SLOT[part])
            if rnd == 0:
                landed(gcf, 3)
            close_sweep(rnd, ghost_accs, gcf, ghost_start, FAR)

        @pl.when(plain)
        def _():
            table_here(rnd + 1, partner)

        for n, part in enumerate(fast_order):
            if n:
                table_here(rnd + 1, part)
            add(part)
        if not final:
            close_sweep(rnd + 1, accs, cf, own_start, OWN)

    for i, w in enumerate(where):
        mixed = None
        for c in range(3):
            v = tan2[c * erow + i * 8 : c * erow + i * 8 + 8, :] * (tacc[i][c + 1] + hacc[i][c + 1])
            mixed = v if mixed is None else mixed + v
        out_ref[w, :] = scale[w, :] * res[w, :] + ((hacc[i][0] - tacc[i][0]) + 0.5 * mixed)

    pl.when(g != G - 1)(parts_left)
    left(part_rows(psend, FAR), 9)
    left(got_send, 1)

    @pl.when(seam)
    def _():
        left(cf, 2)
        left(sq, 3)

    for rnd in range(SWEEPS):
        counts = ((inner, 4), (feeds, 5), (seam, 6)) if rnd % 2 == 0 else ((plain, 4), (seam, 3))
        for which, n in counts:
            pl.when(which)(lambda n=n: left(tab.at[rnd, pl.ds(0, n * vrow)], 4 + rnd))


def body(
    residual, edge_scale, tangent, edge_tail, edge_head,
    stencil_index, stencil_coef, diag_margin, send_index,
):
    edges = residual.shape[0]
    erow = edges // LANES
    nodes = diag_margin.shape[1]
    nrow = nodes // LANES
    vrow = 4 * nrow
    stencil = stencil_index.shape[0]
    qrow = -(-stencil * nrow // 8) * 8
    assert send_index.shape == (2, 2, nodes) and lax.axis_size("grp") % 2 == 0 and lax.axis_size("grp") > 4
    coef = jnp.transpose(stencil_coef, (1, 0, 2))
    square = lambda x: x.reshape(erow, LANES)
    anyspace = pl.BlockSpec(memory_space=pl.ANY)
    vm = pltpu.VMEM
    dma = pltpu.SemaphoreType.DMA
    out = pl.pallas_call(
        kernel,
        out_shape=vm((erow, LANES), F32),
        in_specs=[anyspace] * 9,
        out_specs=pl.BlockSpec(memory_space=vm),
        scratch_shapes=[
            vm((erow, LANES), F32),
            vm(tangent.shape, F32),
            vm((erow, LANES), I32),
            vm((erow, LANES), I32),
            vm(stencil_index.shape, I32),
            vm(coef.shape, BF16),
            vm(diag_margin.shape, F32),
            vm(send_index.shape, I32),
            vm((erow, LANES), F32),
            vm((4,) + send_index.shape, I32),
            vm((8 * vrow, LANES), F32),
            vm((8 * vrow, LANES), F32),
            vm((SWEEPS, SLOTS * vrow, LANES), F32),
            vm((LANES, edges), BF16),
            vm((2 * vrow, edges), BF16),
            vm((4 * vrow, edges), BF16),
            vm((14 * vrow, edges), BF16),
            vm((LANES, 4 * nodes), BF16),
            vm((2 * vrow, 4 * nodes), BF16),
            vm((4 * vrow, LANES), F32),
            vm((4, qrow, LANES), F32),
            vm((4, qrow, LANES), F32),
            vm((vrow, LANES), F32),
            vm((vrow, LANES), F32),
            vm((erow, LANES), I32),
            vm((erow, LANES), I32),
            vm((qrow, LANES), I32),
            vm((qrow, LANES), I32),
            vm((3 * erow, LANES), F32),
            dma((10,)),
            dma((5 + 9 * (SWEEPS // 2),)),
        ],
        compiler_params=pltpu.CompilerParams(collective_id=0, has_side_effects=True),
    )(
        square(residual), tangent, square(edge_tail), square(edge_head),
        stencil_index, coef, diag_margin, send_index, square(edge_scale),
    )
    return out.reshape(edges)


def solution(mesh):
    return jax.shard_map(
        body,
        mesh=mesh,
        in_specs=(
            P(("grp", "sub")),
            P(("grp", "sub")),
            P(None, ("grp", "sub")),
            P(("grp", "sub")),
            P(("grp", "sub")),
            P(None, ("grp", "sub")),
            P(None, None, ("grp", "sub")),
            P(None, ("grp", "sub")),
            P("grp", "sub", None),
        ),
        out_specs=P(("grp", "sub")),
        check_vma=False,
    )
```

```python
import jax
import jax.numpy as jnp
from jax import lax
from jax.experimental import pallas as pl
from jax.experimental.pallas import tpu as pltpu
from jax.sharding import PartitionSpec as P

SWEEPS = 4
LANES = 128
SLOTS = 8
MESH = pl.DeviceIdType.MESH
DNUMS = lax.GatherDimensionNumbers(
    offset_dims=(),
    collapsed_slice_dims=(1,),
    start_index_map=(1,),
    operand_batching_dims=(0,),
    start_indices_batching_dims=(0,),
)
F32 = jnp.float32
BF16 = jnp.bfloat16
I32 = jnp.int32

OWN, FAR, NEAR, SM, SP = range(5)
FAR_NEAR, FAR_SM, FAR_SP = 5, 6, 7
GHOST_SLOT = (FAR, OWN, FAR_NEAR, FAR_SM, FAR_SP)


def lane_gather(table, lane):
    return lax.gather(
        table,
        lane[..., None],
        DNUMS,
        slice_sizes=(1, 1),
        mode=lax.GatherScatterMode.PROMISE_IN_BOUNDS,
    )


def nt_dot(a, b):
    return lax.dot_general(a, b, (((1,), (1,)), ((), ())), preferred_element_type=F32)


def kernel(
    res_h, tan_h, tail_h, head_h, sidx_h, coef_h, marg_h, send_h, scale_h,
    out_ref,
    res, tan, tail, head, sidx, coef, marg, own_send, scale,
    got_send, psend, got_p, tab, onehot, spread_o, spread_f, spread_r, onehot3, spread3, tsum,
    cf, gcf, bsc, diag, hq, hl, sq, gq, sidx2, gacc, tan2, relay_p, relay_l,
    send_sem, recv_sem,
):
    G, S = lax.axis_size("grp"), lax.axis_size("sub")
    g, s = lax.axis_index("grp"), lax.axis_index("sub")
    odd = lax.rem(g, 2)
    even = 1 - odd
    gf, gn = lax.rem(g + G - 1 + 2 * odd, G), lax.rem(g + 1 + (G - 2) * odd, G)
    sm, sp = lax.rem(s + S - 1, S), lax.rem(s + 1, S)
    peer = {FAR: (gf, s), NEAR: (gn, s), SM: (g, sm), SP: (g, sp)}
    nn_to = (lax.rem(g + 2 + (G - 4) * odd, G), s)
    seam = (g == 0) | (g == G - 1)
    plain = (g != 0) & (g != G - 1)
    feeds = (g == 1) | (g == G - 2)
    inner = plain & (g != 1) & (g != G - 2)
    s_odd = lax.rem(s, 2)
    paired = (g, s + 1 - 2 * s_odd)
    lead = (g == 0) & (s_odd == 0)
    led = (g != 0) | (s_odd != 0)
    aide = (g == 0) & (s_odd == 1)
    far_aide = (g == G - 1) & (s_odd == 1)
    either_aide = seam & (s_odd == 1)
    back = {FAR: FAR, NEAR: NEAR, SM: SP, SP: SM}
    nrow = marg.shape[1] // LANES
    erow = res.shape[0]
    stencil = sidx.shape[0]
    vrow = 4 * nrow
    sent = 2 * vrow
    tiles = [slice(i * 8, i * 8 + 8) for i in range(sq.shape[0] // 8)]

    barrier = pltpu.get_barrier_semaphore()
    for o in (NEAR, SM, SP):
        pl.semaphore_signal(barrier, inc=1, device_id=peer[o], device_id_type=MESH)

    skip = (g == G - 1) & (s_odd == 0)
    greeted = (jnp.where(skip, lax.rem(g + 2, G), gf), s)
    pl.semaphore_signal(barrier, inc=1, device_id=greeted, device_id_type=MESH)

    pairs = (
        (head_h, head, 0), (res_h, res, 4), (tan_h, tan, 5), (send_h, own_send, 1), (tail_h, tail, 2),
        (coef_h, coef, 3), (marg_h, marg, 6), (sidx_h, sidx, 7), (scale_h, scale, 8),
    )
    local = [pltpu.make_async_copy(src, dst, send_sem.at[i]) for src, dst, i in pairs]
    for c in local:
        c.start()

    def copy_to(src, dst, ssem, rsem, who):
        return pltpu.make_async_remote_copy(
            src_ref=src, dst_ref=dst, send_sem=send_sem.at[ssem], recv_sem=recv_sem.at[rsem],
            device_id=who, device_id_type=MESH,
        )

    def landed(dst, rsem):
        copy_to(dst, dst, 0, rsem, peer[SP]).wait_recv()

    def left(src, ssem):
        copy_to(src, src, ssem, 0, peer[SP]).wait_send()

    def part_rows(ref, o):
        return ref.at[pl.ds((o - 1) * sent, sent)]

    def send_part(o):
        far = o == FAR
        copy_to(part_rows(psend, o), part_rows(got_p, back[o]), 9 if far else 0, 0 if far else 1, peer[o]).start()

    def send_list(o):
        copy_to(own_send, got_send.at[back[o] - 1], 1, 25 if o == FAR else 2, peer[o]).start()

    def slot_rows(rnd, slot):
        return tab.at[rnd, pl.ds(slot * vrow, vrow)]

    def table_sem(rnd, slot):
        slot = min(slot, FAR_NEAR) if isinstance(slot, int) else slot
        return 5 + 9 * (rnd // 2) + slot - 1 + FAR_NEAR * (rnd % 2)

    def send_table(rnd, who, slot):
        copy_to(slot_rows(rnd, OWN), slot_rows(rnd, slot), 4 + rnd, table_sem(rnd, slot), who).start()

    def table_here(rnd, first, count=1):
        landed(tab.at[rnd, pl.ds(first * vrow, count * vrow)], table_sem(rnd, first))

    riota = lax.broadcasted_iota(I32, (vrow, LANES), 0)
    kind = riota // nrow
    rpart = (riota - kind * nrow).astype(F32).astype(BF16)
    lane16 = lax.broadcasted_iota(I32, (16, LANES), 0).astype(F32).astype(BF16)
    one, zero = jnp.ones((), BF16), jnp.zeros((), BF16)

    def cols_of(t):
        return slice(t * LANES, (t + 1) * LANES)

    def wide(row, rows):
        return jnp.broadcast_to(row.astype(F32), (rows, LANES)).astype(BF16)

    def lanes_onehot(ref, cols, x):
        lane = wide(x & (LANES - 1), 16)
        for q in range(LANES // 16):
            mine = lane16 + jnp.full((), 16 * q, BF16)
            ref[q * 16 : q * 16 + 16, cols] = jnp.where(mine == lane, one, zero)

    def split(val):
        hi = val.astype(BF16)
        return hi, (val - hi.astype(F32)).astype(BF16)

    def terms(t, sign):
        r = res[t : t + 1, :]
        val = jnp.broadcast_to(r if sign > 0 else -r, (vrow, LANES))
        half = 0.5 * r
        for c in range(3):
            val = jnp.where(kind == c + 1, tan[c : c + 1, cols_of(t)] * half, val)
        return split(val)

    def scatter(ref, rows_of, bases, sign, make=None):
        n = len(bases)
        for t in range(erow):
            cols = cols_of(t)
            x = rows_of[t : t + 1, :]
            if make:
                lanes_onehot(onehot, cols, x)
            pieces = terms(t, sign)
            row = wide(x >> 7, vrow)
            for j, base in enumerate(bases):
                hit = row == rpart + base
                for p, v in enumerate(pieces):
                    at = (p * n + j) * vrow
                    ref[at : at + vrow, cols] = jnp.where(hit, v, zero)
        both = nt_dot(ref[...], onehot[...])
        return both[: n * vrow] + both[n * vrow :]

    def base_of(block):
        return (jnp.asarray(block, I32) * nrow).astype(F32).astype(BF16)

    far_block, near_block = 1 + 2 * odd, 3 - 2 * odd

    for c in local[:4]:
        c.wait()
    psend[0:sent] = scatter(spread_f, head, [base_of(far_block), base_of(far_block + 1)], 1, make=True)

    def first_sends():
        extra = (g == 1) & (s_odd == 0)
        pl.semaphore_wait(barrier, jnp.where(lead, 3, jnp.where(extra, 5, 4)))

        @pl.when(lead)
        def _():
            copy_to(part_rows(psend, FAR), relay_p, 9, 23, paired).start()
            copy_to(own_send, relay_l, 1, 24, paired).start()

        @pl.when(aide)
        def _():
            landed(relay_p, 23)
            copy_to(relay_p, relay_p, 10, 23, peer[FAR]).start()
            landed(relay_l, 24)
            copy_to(relay_l, relay_l, 11, 24, peer[FAR]).start()

        @pl.when(led)
        def _():
            send_part(FAR)
            send_list(FAR)

        for o in (NEAR, SM, SP):
            send_list(o)

    pl.when(g != 0)(first_sends)
    rest = scatter(
        spread_r, head,
        [base_of(b) for b in (near_block, near_block + 1, 5, 6, 7, 8, 0)], 1,
    )
    psend[sent:] = rest[: 3 * sent]
    own_sum = rest[3 * sent :]
    pl.when(g == 0)(first_sends)
    for o in (NEAR, SM, SP):
        send_part(o)
    for c in local[4:]:
        c.wait()

    if cf.shape[1] > stencil * nrow:
        cf[...] = jnp.zeros_like(cf)
        sidx2[...] = jnp.zeros_like(sidx2)
    for k in range(4):
        for r in range(nrow):
            cols = cols_of(r)
            c = coef[:, k, cols].astype(F32)
            d = (1.0 + marg[k : k + 1, cols]) * jnp.sum(jnp.abs(c), axis=0, keepdims=True)
            inv = 1.0 / d
            diag[k * nrow + r : k * nrow + r + 1, :] = inv
            cf[k, pl.ds(r, stencil, stride=nrow), :] = c * inv

    for t in range(erow):
        lanes_onehot(onehot, cols_of(t), tail[t : t + 1, :])
    own_sum = own_sum + scatter(spread_o, tail, [base_of(0)], -1)

    a_of = (odd, even)
    lists = tuple((f, b, r) for f in range(2) for b in range(2) for r in range(nrow))

    def own_list(f, b, r):
        return own_send[a_of[f], b : b + 1, cols_of(r)]

    for n, fbr in enumerate(lists):
        lanes_onehot(onehot3, cols_of(n), own_list(*fbr))
    for c in range(3):
        for t in range(erow):
            tan2[c * erow + t : c * erow + t + 1, :] = tan[c : c + 1, cols_of(t)]
    for r in range(nrow):
        sidx2[pl.ds(r, stencil, stride=nrow), :] = sidx[:, cols_of(r)]

    def place(ref, at, f, b, r):
        hit = wide(own_list(f, b, r) >> 7, vrow) == rpart
        base = b * vrow + r + at
        val = jnp.broadcast_to(ref[base : base + 1, :], (vrow, LANES))
        for k in range(1, 4):
            row = base + k * nrow
            val = jnp.where(kind == k, ref[row : row + 1, :], val)
        return [jnp.where(hit, v, zero) for v in split(val)]

    parts_left = lambda: left(psend.at[pl.ds(sent, 3 * sent)], 0)
    pl.when(g == G - 1)(parts_left)

    def send_factor():
        copy_to(cf, gcf, 2, 3, peer[FAR]).start()

    pl.when(seam & led)(send_factor)

    @pl.when(far_aide)
    def _():
        landed(relay_p, 23)
        copy_to(relay_p, part_rows(got_p, FAR), 10, 0, paired).start()
        landed(relay_l, 24)
        copy_to(relay_l, got_send.at[FAR - 1], 11, 25, paired).start()

    landed(got_p.at[pl.ds(sent, 3 * sent)], 1)
    for f in range(2):
        for b in range(2):
            first = pl.multiple_of((2 + b) * sent + a_of[f] * vrow, vrow)
            val = got_p[pl.ds(first, vrow), :]
            if f:
                val = val + got_p[sent + b * vrow : sent + (b + 1) * vrow, :]
            at = (f * 2 + b) * vrow
            tsum[at : at + vrow, :] = val
    for n, (f, b, r) in enumerate(lists):
        for p, v in enumerate(place(tsum, f * sent, f, b, r)):
            spread3[p * vrow : (p + 1) * vrow, cols_of(n)] = v
    got = nt_dot(spread3[...], onehot3[...])
    own_sum = own_sum + (got[:vrow] + got[vrow:])

    def compose(x, y, parts):
        lane = x & (LANES - 1)
        row = x >> 7
        for o in parts:
            block = {FAR: far_block, NEAR: near_block, SM: 5, SP: 7}[o]
            for h in range(2):
                a, b = {FAR: (even, h), NEAR: (odd, h), SM: (h, 1), SP: (h, 0)}[o]
                for r in range(nrow):
                    line = got_send[o - 1, a, b : b + 1, cols_of(r)]
                    line = jnp.broadcast_to(line + o * nrow * LANES, x.shape)
                    y = jnp.where(row == (block + h) * nrow + r, lane_gather(line, lane), y)
        return y

    landed(got_send.at[pl.ds(NEAR - 1, 3)], 2)
    for w in tiles:
        sq[w, :] = compose(sidx2[w, :], sidx2[w, :], (NEAR, SM, SP))

    landed(part_rows(got_p, FAR), 0)
    half = len(lists) // 2
    for n, (f, b, r) in enumerate(lists[:half]):
        for p, v in enumerate(place(got_p, 0, f, b, r)):
            spread3[p * vrow : (p + 1) * vrow, cols_of(n)] = v
    got = nt_dot(spread3[:, : half * LANES], onehot3[:, : half * LANES])
    bsc[...] = (own_sum + (got[:vrow] + got[vrow:])) * diag[...]
    tab[0, :vrow, :] = bsc[...]

    def send_round(rnd, deep):
        if deep:
            send_table(rnd, peer[FAR], FAR)
        for o in (NEAR, SM, SP):
            send_table(rnd, peer[o], back[o])
        if deep:
            @pl.when(seam)
            def _():
                send_table(rnd, (gf, sp), FAR_SM)
                send_table(rnd, (gf, sm), FAR_SP)

            @pl.when(feeds)
            def _():
                send_table(rnd, nn_to, FAR_NEAR)
        else:
            @pl.when(plain)
            def _():
                send_table(rnd, peer[FAR], FAR)

    def compose_far():
        landed(got_send.at[FAR - 1], 25)
        for w in tiles:
            sq[w, :] = compose(sidx2[w, :], sq[w, :], (FAR,))

        @pl.when(seam)
        def _():
            copy_to(sq, gq, 3, 4, peer[FAR]).start()

        pl.when(lead)(send_factor)

    def compose_heads():
        for i in range(erow // 8):
            x = head[i * 8 : i * 8 + 8, :]
            y = compose(x, x, (FAR, NEAR, SM, SP))
            hq[i * 8 : i * 8 + 8, :] = y >> 7
            hl[i * 8 : i * 8 + 8, :] = y & (LANES - 1)

    def add_rows(rnd, slot, part, rows, lanes, accs):
        for i in range(len(rows)):
            for r in range(nrow):
                hit = rows[i] == part * nrow + r
                for k in range(4):
                    at = slot * vrow + k * nrow + r
                    line = jnp.broadcast_to(tab[rnd, pl.ds(at, 1), :], rows[i].shape)
                    v = lane_gather(line, lanes[i])
                    accs[i][k] = v if accs[i][k] is None else jnp.where(hit, v, accs[i][k])

    sub8 = lax.broadcasted_iota(I32, (8, LANES), 0)

    def open_sweep(rnd, index):
        where = [index[w, :] for w in tiles]
        rows = [y >> 7 for y in where]
        lanes = [y & (LANES - 1) for y in where]
        accs = [[None] * 4 for _ in tiles]

        def add(part, slot=None):
            add_rows(rnd, part if slot is None else slot, part, rows, lanes, accs)

        return add, accs

    def close_sweep(rnd, accs, factor, start, out_slot):
        totals = []
        for k in range(4):
            total = None
            for w, acc in zip(tiles, accs):
                v = acc[k] * factor[k, w, :]
                total = v if total is None else total + v
            step = nrow
            while step < 8:
                total = total + pltpu.roll(total, step, axis=0)
                step *= 2
            totals.append(total)
        for at in range(0, vrow, 8):
            total = totals[at // nrow]
            for m in range(1, 8 // nrow):
                total = jnp.where(sub8 >= m * nrow, totals[at // nrow + m], total)
            to = out_slot * vrow + at
            tab[rnd + 1, to : to + 8, :] = start(at) - total

    def own_start(at):
        return bsc[at : at + 8, :]

    def ghost_start(at):
        return tab[0, FAR * vrow + at : FAR * vrow + at + 8, :]

    partner, across = SP - s_odd, SM + s_odd
    second, third = SM - s_odd, NEAR + 2 * s_odd

    def either(here, there):
        return [jnp.where(seam, a, b) for a, b in zip(here, there)]

    slow_order = (
        either((partner, second, third, FAR), (partner, across, FAR, NEAR)),
        either((partner, second, FAR, third), (partner, across, FAR, NEAR)),
    )
    late_order = either((partner, second, third, FAR), (partner, across, FAR, NEAR))
    early_order = either((FAR, partner, second, third), (partner, across, FAR, NEAR))

    for rnd in range(0, SWEEPS, 2):
        send_round(rnd, True)
        if rnd == 0:
            compose_far()
            compose_heads()
        add, accs = open_sweep(rnd, sq)
        add(OWN)
        for part in slow_order[rnd // 2]:
            table_here(rnd, part)
            add(part)
        close_sweep(rnd, accs, cf, own_start, OWN)
        send_round(rnd + 1, False)

        final = rnd + 2 == SWEEPS
        if final:
            where = [slice(i * 8, i * 8 + 8) for i in range(erow // 8)]
            tails = [tail[w, :] for w in where]
            tacc = [[None] * 4 for _ in where]
            add_rows(rnd + 1, OWN, OWN, [t >> 7 for t in tails], [t & (LANES - 1) for t in tails], tacc)
            rows = [hq[w, :] for w in where]
            lanes = [hl[w, :] for w in where]
            hacc = [[None] * 4 for _ in where]

            def add(part):
                add_rows(rnd + 1, part, part, rows, lanes, hacc)
        else:
            add, accs = open_sweep(rnd + 1, sq)
        add(OWN)

        def ghost_tables():
            if rnd == 0:
                landed(gq, 4)
            ghost_add, ghost_accs = open_sweep(rnd, gq)
            ghost_add(OWN, FAR)
            ghost_add(FAR, OWN)
            table_here(rnd, FAR_NEAR, 3)
            for part in (NEAR, SM, SP):
                ghost_add(part, GHOST_SLOT[part])
            return ghost_accs

        def ghost_begin():
            for n, v in enumerate(sum(ghost_tables(), [])):
                gacc[n * 8 : n * 8 + 8, :] = v

        def ghost_end():
            landed(gcf, 3)
            held = [[gacc[n * 8 : n * 8 + 8, :] for n in range(4 * i, 4 * i + 4)] for i in range(len(tiles))]
            close_sweep(rnd, held, gcf, ghost_start, FAR)

        def ghost_whole():
            close_sweep(rnd, ghost_tables(), gcf, ghost_start, FAR)

        if not final:
            pl.when(seam)(ghost_begin)
            for n, part in enumerate(late_order):
                if n < 3:
                    table_here(rnd + 1, part)
                else:
                    pl.when(seam)(ghost_end)
                    pl.when(plain)(lambda: table_here(rnd + 1, NEAR))
                add(part)
        else:
            pl.when(seam)(ghost_whole)
            pl.when(plain)(lambda: table_here(rnd + 1, partner))
            for n, part in enumerate(early_order):
                if n:
                    table_here(rnd + 1, part)
                add(part)
        if not final:
            close_sweep(rnd + 1, accs, cf, own_start, OWN)

    for i, w in enumerate(where):
        mixed = None
        for c in range(3):
            v = tan2[c * erow + i * 8 : c * erow + i * 8 + 8, :] * (tacc[i][c + 1] + hacc[i][c + 1])
            mixed = v if mixed is None else mixed + v
        out_ref[w, :] = scale[w, :] * res[w, :] + ((hacc[i][0] - tacc[i][0]) + 0.5 * mixed)

    pl.when(g != G - 1)(parts_left)
    left(part_rows(psend, FAR), 9)
    left(got_send, 1)

    @pl.when(seam)
    def _():
        left(cf, 2)
        left(sq, 3)

    @pl.when(either_aide)
    def _():
        left(relay_p, 10)
        left(relay_l, 11)

    for rnd in range(SWEEPS):
        counts = ((inner, 4), (feeds, 5), (seam, 6)) if rnd % 2 == 0 else ((plain, 4), (seam, 3))
        for which, n in counts:
            pl.when(which)(lambda n=n: left(tab.at[rnd, pl.ds(0, n * vrow)], 4 + rnd))


def body(
    residual, edge_scale, tangent, edge_tail, edge_head,
    stencil_index, stencil_coef, diag_margin, send_index,
):
    edges = residual.shape[0]
    erow = edges // LANES
    nodes = diag_margin.shape[1]
    nrow = nodes // LANES
    vrow = 4 * nrow
    stencil = stencil_index.shape[0]
    qrow = -(-stencil * nrow // 8) * 8
    assert send_index.shape == (2, 2, nodes) and lax.axis_size("grp") % 2 == 0 and lax.axis_size("grp") > 4 and lax.axis_size("sub") % 2 == 0
    coef = jnp.transpose(stencil_coef, (1, 0, 2))
    square = lambda x: x.reshape(erow, LANES)
    anyspace = pl.BlockSpec(memory_space=pl.ANY)
    vm = pltpu.VMEM
    dma = pltpu.SemaphoreType.DMA
    out = pl.pallas_call(
        kernel,
        out_shape=vm((erow, LANES), F32),
        in_specs=[anyspace] * 9,
        out_specs=pl.BlockSpec(memory_space=vm),
        scratch_shapes=[
            vm((erow, LANES), F32),
            vm(tangent.shape, F32),
            vm((erow, LANES), I32),
            vm((erow, LANES), I32),
            vm(stencil_index.shape, I32),
            vm(coef.shape, BF16),
            vm(diag_margin.shape, F32),
            vm(send_index.shape, I32),
            vm((erow, LANES), F32),
            vm((4,) + send_index.shape, I32),
            vm((8 * vrow, LANES), F32),
            vm((8 * vrow, LANES), F32),
            vm((SWEEPS, SLOTS * vrow, LANES), F32),
            vm((LANES, edges), BF16),
            vm((2 * vrow, edges), BF16),
            vm((4 * vrow, edges), BF16),
            vm((14 * vrow, edges), BF16),
            vm((LANES, 4 * nodes), BF16),
            vm((2 * vrow, 4 * nodes), BF16),
            vm((4 * vrow, LANES), F32),
            vm((4, qrow, LANES), F32),
            vm((4, qrow, LANES), F32),
            vm((vrow, LANES), F32),
            vm((vrow, LANES), F32),
            vm((erow, LANES), I32),
            vm((erow, LANES), I32),
            vm((qrow, LANES), I32),
            vm((qrow, LANES), I32),
            vm((qrow, LANES), I32),
            vm((4 * qrow, LANES), F32),
            vm((3 * erow, LANES), F32),
            vm((2 * vrow, LANES), F32),
            vm(send_index.shape, I32),
            dma((12,)),
            dma((8 + 9 * (SWEEPS // 2),)),
        ],
        compiler_params=pltpu.CompilerParams(collective_id=0, has_side_effects=True),
    )(
        square(residual), tangent, square(edge_tail), square(edge_head),
        stencil_index, coef, diag_margin, send_index, square(edge_scale),
    )
    return out.reshape(edges)


def solution(mesh):
    return jax.shard_map(
        body,
        mesh=mesh,
        in_specs=(
            P(("grp", "sub")),
            P(("grp", "sub")),
            P(None, ("grp", "sub")),
            P(("grp", "sub")),
            P(("grp", "sub")),
            P(None, ("grp", "sub")),
            P(None, None, ("grp", "sub")),
            P(None, ("grp", "sub")),
            P("grp", "sub", None),
        ),
        out_specs=P(("grp", "sub")),
        check_vma=False,
    )
```

```python
import jax
import jax.numpy as jnp
from jax import lax
from jax.experimental import pallas as pl
from jax.experimental.pallas import tpu as pltpu
from jax.sharding import PartitionSpec as P

SWEEPS = 4
LANES = 128
SLOTS = 8
MESH = pl.DeviceIdType.MESH
DNUMS = lax.GatherDimensionNumbers(
    offset_dims=(),
    collapsed_slice_dims=(1,),
    start_index_map=(1,),
    operand_batching_dims=(0,),
    start_indices_batching_dims=(0,),
)
F32 = jnp.float32
BF16 = jnp.bfloat16
I32 = jnp.int32

OWN, FAR, NEAR, SM, SP = range(5)
FAR_NEAR, FAR_SM, FAR_SP = 5, 6, 7
GHOST_SLOT = (FAR, OWN, FAR_NEAR, FAR_SM, FAR_SP)


def lane_gather(table, lane):
    return lax.gather(
        table,
        lane[..., None],
        DNUMS,
        slice_sizes=(1, 1),
        mode=lax.GatherScatterMode.PROMISE_IN_BOUNDS,
    )


def nt_dot(a, b):
    return lax.dot_general(a, b, (((1,), (1,)), ((), ())), preferred_element_type=F32)


def kernel(
    res_h, tan_h, tail_h, head_h, sidx_h, coef_h, marg_h, send_h, scale_h,
    out_ref,
    res, tan, tail, head, sidx, coef, marg, own_send, scale,
    got_send, psend, got_p, tab, onehot, spread_o, spread_f, spread_r, onehot3, spread3, tsum,
    cf, gcf, bsc, diag, hq, hl, sq, gq, sidx2, gacc, tan2, relay_p, relay_l,
    send_sem, recv_sem,
):
    G, S = lax.axis_size("grp"), lax.axis_size("sub")
    g, s = lax.axis_index("grp"), lax.axis_index("sub")
    odd = lax.rem(g, 2)
    even = 1 - odd
    gf, gn = lax.rem(g + G - 1 + 2 * odd, G), lax.rem(g + 1 + (G - 2) * odd, G)
    sm, sp = lax.rem(s + S - 1, S), lax.rem(s + 1, S)
    peer = {FAR: (gf, s), NEAR: (gn, s), SM: (g, sm), SP: (g, sp)}
    nn_to = (lax.rem(g + 2 + (G - 4) * odd, G), s)
    seam = (g == 0) | (g == G - 1)
    plain = (g != 0) & (g != G - 1)
    feeds = (g == 1) | (g == G - 2)
    inner = plain & (g != 1) & (g != G - 2)
    s_odd = lax.rem(s, 2)
    paired = (g, s + 1 - 2 * s_odd)
    lead = (g == 0) & (s_odd == 0)
    led = (g != 0) | (s_odd != 0)
    aide = (g == 0) & (s_odd == 1)
    far_aide = (g == G - 1) & (s_odd == 1)
    either_aide = seam & (s_odd == 1)
    back = {FAR: FAR, NEAR: NEAR, SM: SP, SP: SM}
    nrow = marg.shape[1] // LANES
    erow = res.shape[0]
    stencil = sidx.shape[0]
    vrow = 4 * nrow
    sent = 2 * vrow
    tiles = [slice(i * 8, i * 8 + 8) for i in range(sq.shape[0] // 8)]

    barrier = pltpu.get_barrier_semaphore()
    for o in (NEAR, SM, SP):
        pl.semaphore_signal(barrier, inc=1, device_id=peer[o], device_id_type=MESH)

    skip = (g == G - 1) & (s_odd == 0)
    greeted = (jnp.where(skip, lax.rem(g + 2, G), gf), s)
    pl.semaphore_signal(barrier, inc=1, device_id=greeted, device_id_type=MESH)

    pairs = (
        (head_h, head, 0), (res_h, res, 4), (tan_h, tan, 5), (send_h, own_send, 1), (tail_h, tail, 2),
        (coef_h, coef, 3), (marg_h, marg, 6), (sidx_h, sidx, 7), (scale_h, scale, 8),
    )
    local = [pltpu.make_async_copy(src, dst, send_sem.at[i]) for src, dst, i in pairs]
    for c in local:
        c.start()

    def copy_to(src, dst, ssem, rsem, who):
        return pltpu.make_async_remote_copy(
            src_ref=src, dst_ref=dst, send_sem=send_sem.at[ssem], recv_sem=recv_sem.at[rsem],
            device_id=who, device_id_type=MESH,
        )

    def landed(dst, rsem):
        copy_to(dst, dst, 0, rsem, peer[SP]).wait_recv()

    def left(src, ssem):
        copy_to(src, src, ssem, 0, peer[SP]).wait_send()

    def part_rows(ref, o):
        return ref.at[pl.ds((o - 1) * sent, sent)]

    def send_part(o):
        far = o == FAR
        copy_to(part_rows(psend, o), part_rows(got_p, back[o]), 9 if far else 0, 0 if far else 1, peer[o]).start()

    def send_list(o):
        copy_to(own_send, got_send.at[back[o] - 1], 1, 25 if o == FAR else 2, peer[o]).start()

    def slot_rows(rnd, slot):
        return tab.at[rnd, pl.ds(slot * vrow, vrow)]

    def table_sem(rnd, slot):
        slot = min(slot, FAR_NEAR) if isinstance(slot, int) else slot
        return 5 + 9 * (rnd // 2) + slot - 1 + FAR_NEAR * (rnd % 2)

    def send_table(rnd, who, slot):
        copy_to(slot_rows(rnd, OWN), slot_rows(rnd, slot), 4 + rnd, table_sem(rnd, slot), who).start()

    def table_here(rnd, first, count=1):
        landed(tab.at[rnd, pl.ds(first * vrow, count * vrow)], table_sem(rnd, first))

    riota = lax.broadcasted_iota(I32, (vrow, LANES), 0)
    kind = riota // nrow
    rpart = (riota - kind * nrow).astype(F32).astype(BF16)
    lane16 = lax.broadcasted_iota(I32, (16, LANES), 0).astype(F32).astype(BF16)
    one, zero = jnp.ones((), BF16), jnp.zeros((), BF16)

    def cols_of(t):
        return slice(t * LANES, (t + 1) * LANES)

    def wide(row, rows):
        return jnp.broadcast_to(row.astype(F32), (rows, LANES)).astype(BF16)

    def lanes_onehot(ref, cols, x):
        lane = wide(x & (LANES - 1), 16)
        for q in range(LANES // 16):
            mine = lane16 + jnp.full((), 16 * q, BF16)
            ref[q * 16 : q * 16 + 16, cols] = jnp.where(mine == lane, one, zero)

    def split(val):
        hi = val.astype(BF16)
        return hi, (val - hi.astype(F32)).astype(BF16)

    def terms(t, sign):
        r = res[t : t + 1, :]
        val = jnp.broadcast_to(r if sign > 0 else -r, (vrow, LANES))
        half = 0.5 * r
        for c in range(3):
            val = jnp.where(kind == c + 1, tan[c : c + 1, cols_of(t)] * half, val)
        return split(val)

    def scatter(ref, rows_of, bases, sign, make=None):
        n = len(bases)
        for t in range(erow):
            cols = cols_of(t)
            x = rows_of[t : t + 1, :]
            if make:
                lanes_onehot(onehot, cols, x)
            pieces = terms(t, sign)
            row = wide(x >> 7, vrow)
            for j, base in enumerate(bases):
                hit = row == rpart + base
                for p, v in enumerate(pieces):
                    at = (p * n + j) * vrow
                    ref[at : at + vrow, cols] = jnp.where(hit, v, zero)
        both = nt_dot(ref[...], onehot[...])
        return both[: n * vrow] + both[n * vrow :]

    def base_of(block):
        return (jnp.asarray(block, I32) * nrow).astype(F32).astype(BF16)

    far_block, near_block = 1 + 2 * odd, 3 - 2 * odd

    for c in local[:4]:
        c.wait()
    psend[0:sent] = scatter(spread_f, head, [base_of(far_block), base_of(far_block + 1)], 1, make=True)

    extra = (g == 1) & (s_odd == 0)

    def first_sends():
        pl.semaphore_wait(barrier, jnp.where(lead, 3, jnp.where(extra, 5, 4)))

        @pl.when(lead)
        def _():
            copy_to(part_rows(psend, FAR), relay_p, 9, 23, paired).start()
            copy_to(own_send, relay_l, 1, 24, paired).start()

        @pl.when(aide)
        def _():
            landed(relay_p, 23)
            copy_to(relay_p, relay_p, 10, 23, peer[FAR]).start()
            landed(relay_l, 24)
            copy_to(relay_l, relay_l, 11, 24, peer[FAR]).start()

        @pl.when(led)
        def _():
            send_part(FAR)
            send_list(FAR)

        for o in (NEAR, SM, SP):
            send_list(o)

    late = (g == 0) | extra
    pl.when(jnp.logical_not(late))(first_sends)
    rest = scatter(
        spread_r, head,
        [base_of(b) for b in (near_block, near_block + 1, 5, 6, 7, 8, 0)], 1,
    )
    psend[sent:] = rest[: 3 * sent]
    own_sum = rest[3 * sent :]
    pl.when(late)(first_sends)
    for o in (NEAR, SM, SP):
        send_part(o)
    for c in local[4:]:
        c.wait()

    if cf.shape[1] > stencil * nrow:
        cf[...] = jnp.zeros_like(cf)
        sidx2[...] = jnp.zeros_like(sidx2)
    for k in range(4):
        for r in range(nrow):
            cols = cols_of(r)
            c = coef[:, k, cols].astype(F32)
            d = (1.0 + marg[k : k + 1, cols]) * jnp.sum(jnp.abs(c), axis=0, keepdims=True)
            inv = 1.0 / d
            diag[k * nrow + r : k * nrow + r + 1, :] = inv
            cf[k, pl.ds(r, stencil, stride=nrow), :] = c * inv

    for t in range(erow):
        lanes_onehot(onehot, cols_of(t), tail[t : t + 1, :])
    own_sum = own_sum + scatter(spread_o, tail, [base_of(0)], -1)

    a_of = (odd, even)
    lists = tuple((f, b, r) for f in range(2) for b in range(2) for r in range(nrow))

    def own_list(f, b, r):
        return own_send[a_of[f], b : b + 1, cols_of(r)]

    for n, fbr in enumerate(lists):
        lanes_onehot(onehot3, cols_of(n), own_list(*fbr))
    for c in range(3):
        for t in range(erow):
            tan2[c * erow + t : c * erow + t + 1, :] = tan[c : c + 1, cols_of(t)]
    for r in range(nrow):
        sidx2[pl.ds(r, stencil, stride=nrow), :] = sidx[:, cols_of(r)]

    def place(ref, at, f, b, r):
        hit = wide(own_list(f, b, r) >> 7, vrow) == rpart
        base = b * vrow + r + at
        val = jnp.broadcast_to(ref[base : base + 1, :], (vrow, LANES))
        for k in range(1, 4):
            row = base + k * nrow
            val = jnp.where(kind == k, ref[row : row + 1, :], val)
        return [jnp.where(hit, v, zero) for v in split(val)]

    parts_left = lambda: left(psend.at[pl.ds(sent, 3 * sent)], 0)
    pl.when(g == G - 1)(parts_left)

    def send_factor():
        copy_to(cf, gcf, 2, 3, peer[FAR]).start()

    pl.when(seam & led)(send_factor)

    @pl.when(far_aide)
    def _():
        landed(relay_p, 23)
        copy_to(relay_p, part_rows(got_p, FAR), 10, 0, paired).start()
        landed(relay_l, 24)
        copy_to(relay_l, got_send.at[FAR - 1], 11, 25, paired).start()

    landed(got_p.at[pl.ds(sent, 3 * sent)], 1)
    for f in range(2):
        for b in range(2):
            first = pl.multiple_of((2 + b) * sent + a_of[f] * vrow, vrow)
            val = got_p[pl.ds(first, vrow), :]
            if f:
                val = val + got_p[sent + b * vrow : sent + (b + 1) * vrow, :]
            at = (f * 2 + b) * vrow
            tsum[at : at + vrow, :] = val
    for n, (f, b, r) in enumerate(lists):
        for p, v in enumerate(place(tsum, f * sent, f, b, r)):
            spread3[p * vrow : (p + 1) * vrow, cols_of(n)] = v
    got = nt_dot(spread3[...], onehot3[...])
    own_sum = own_sum + (got[:vrow] + got[vrow:])

    def compose(x, y, parts):
        lane = x & (LANES - 1)
        row = x >> 7
        for o in parts:
            block = {FAR: far_block, NEAR: near_block, SM: 5, SP: 7}[o]
            for h in range(2):
                a, b = {FAR: (even, h), NEAR: (odd, h), SM: (h, 1), SP: (h, 0)}[o]
                for r in range(nrow):
                    line = got_send[o - 1, a, b : b + 1, cols_of(r)]
                    line = jnp.broadcast_to(line + o * nrow * LANES, x.shape)
                    y = jnp.where(row == (block + h) * nrow + r, lane_gather(line, lane), y)
        return y

    landed(got_send.at[pl.ds(NEAR - 1, 3)], 2)
    for w in tiles:
        sq[w, :] = compose(sidx2[w, :], sidx2[w, :], (NEAR, SM, SP))

    landed(part_rows(got_p, FAR), 0)
    half = len(lists) // 2
    for n, (f, b, r) in enumerate(lists[:half]):
        for p, v in enumerate(place(got_p, 0, f, b, r)):
            spread3[p * vrow : (p + 1) * vrow, cols_of(n)] = v
    got = nt_dot(spread3[:, : half * LANES], onehot3[:, : half * LANES])
    bsc[...] = (own_sum + (got[:vrow] + got[vrow:])) * diag[...]
    tab[0, :vrow, :] = bsc[...]

    def send_round(rnd, deep):
        if deep:
            send_table(rnd, peer[FAR], FAR)
        for o in (NEAR, SM, SP):
            send_table(rnd, peer[o], back[o])
        if deep:
            @pl.when(seam)
            def _():
                send_table(rnd, (gf, sp), FAR_SM)
                send_table(rnd, (gf, sm), FAR_SP)

            @pl.when(feeds)
            def _():
                send_table(rnd, nn_to, FAR_NEAR)
        else:
            @pl.when(plain)
            def _():
                send_table(rnd, peer[FAR], FAR)

    def compose_far():
        landed(got_send.at[FAR - 1], 25)
        for w in tiles:
            sq[w, :] = compose(sidx2[w, :], sq[w, :], (FAR,))

        @pl.when(seam)
        def _():
            copy_to(sq, gq, 3, 4, peer[FAR]).start()

        pl.when(lead)(send_factor)

    def compose_heads():
        for i in range(erow // 8):
            x = head[i * 8 : i * 8 + 8, :]
            y = compose(x, x, (FAR, NEAR, SM, SP))
            hq[i * 8 : i * 8 + 8, :] = y >> 7
            hl[i * 8 : i * 8 + 8, :] = y & (LANES - 1)

    def add_rows(rnd, slot, part, rows, lanes, accs):
        for i in range(len(rows)):
            for r in range(nrow):
                hit = rows[i] == part * nrow + r
                for k in range(4):
                    at = slot * vrow + k * nrow + r
                    line = jnp.broadcast_to(tab[rnd, pl.ds(at, 1), :], rows[i].shape)
                    v = lane_gather(line, lanes[i])
                    accs[i][k] = v if accs[i][k] is None else jnp.where(hit, v, accs[i][k])

    sub8 = lax.broadcasted_iota(I32, (8, LANES), 0)

    def open_sweep(rnd, index):
        where = [index[w, :] for w in tiles]
        rows = [y >> 7 for y in where]
        lanes = [y & (LANES - 1) for y in where]
        accs = [[None] * 4 for _ in tiles]

        def add(part, slot=None):
            add_rows(rnd, part if slot is None else slot, part, rows, lanes, accs)

        return add, accs

    def close_sweep(rnd, accs, factor, start, out_slot):
        totals = []
        for k in range(4):
            total = None
            for w, acc in zip(tiles, accs):
                v = acc[k] * factor[k, w, :]
                total = v if total is None else total + v
            step = nrow
            while step < 8:
                total = total + pltpu.roll(total, step, axis=0)
                step *= 2
            totals.append(total)
        for at in range(0, vrow, 8):
            total = totals[at // nrow]
            for m in range(1, 8 // nrow):
                total = jnp.where(sub8 >= m * nrow, totals[at // nrow + m], total)
            to = out_slot * vrow + at
            tab[rnd + 1, to : to + 8, :] = start(at) - total

    def own_start(at):
        return bsc[at : at + 8, :]

    def ghost_start(at):
        return tab[0, FAR * vrow + at : FAR * vrow + at + 8, :]

    partner, across = SP - s_odd, SM + s_odd
    second, third = SM - s_odd, NEAR + 2 * s_odd

    def either(here, there):
        return [jnp.where(seam, a, b) for a, b in zip(here, there)]

    slow_order = (
        either((partner, second, third, FAR), (partner, across, FAR, NEAR)),
        either((partner, second, third, FAR), (partner, across, NEAR, FAR)),
    )
    late_order = either((partner, second, third, FAR), (partner, across, FAR, NEAR))
    early_order = either((FAR, partner, second, third), (partner, across, FAR, NEAR))

    for rnd in range(0, SWEEPS, 2):
        send_round(rnd, True)
        if rnd == 0:
            compose_far()
            compose_heads()
        add, accs = open_sweep(rnd, sq)
        add(OWN)
        for part in slow_order[rnd // 2]:
            table_here(rnd, part)
            add(part)
        close_sweep(rnd, accs, cf, own_start, OWN)
        send_round(rnd + 1, False)

        final = rnd + 2 == SWEEPS
        if final:
            where = [slice(i * 8, i * 8 + 8) for i in range(erow // 8)]
            tails = [tail[w, :] for w in where]
            tacc = [[None] * 4 for _ in where]
            add_rows(rnd + 1, OWN, OWN, [t >> 7 for t in tails], [t & (LANES - 1) for t in tails], tacc)
            rows = [hq[w, :] for w in where]
            lanes = [hl[w, :] for w in where]
            hacc = [[None] * 4 for _ in where]

            def add(part):
                add_rows(rnd + 1, part, part, rows, lanes, hacc)
        else:
            add, accs = open_sweep(rnd + 1, sq)
        add(OWN)

        def ghost_tables():
            if rnd == 0:
                landed(gq, 4)
            ghost_add, ghost_accs = open_sweep(rnd, gq)
            ghost_add(OWN, FAR)
            ghost_add(FAR, OWN)
            table_here(rnd, FAR_NEAR, 3)
            for part in (NEAR, SM, SP):
                ghost_add(part, GHOST_SLOT[part])
            return ghost_accs

        def ghost_begin():
            for n, v in enumerate(sum(ghost_tables(), [])):
                gacc[n * 8 : n * 8 + 8, :] = v

        def ghost_end():
            landed(gcf, 3)
            held = [[gacc[n * 8 : n * 8 + 8, :] for n in range(4 * i, 4 * i + 4)] for i in range(len(tiles))]
            close_sweep(rnd, held, gcf, ghost_start, FAR)

        def ghost_whole():
            close_sweep(rnd, ghost_tables(), gcf, ghost_start, FAR)

        if not final:
            pl.when(seam)(ghost_begin)
            for n, part in enumerate(late_order):
                if n < 3:
                    table_here(rnd + 1, part)
                else:
                    pl.when(seam)(ghost_end)
                    pl.when(plain)(lambda: table_here(rnd + 1, NEAR))
                add(part)
        else:
            pl.when(seam)(ghost_whole)
            pl.when(plain)(lambda: table_here(rnd + 1, partner))
            for n, part in enumerate(early_order):
                if n:
                    table_here(rnd + 1, part)
                add(part)
        if not final:
            close_sweep(rnd + 1, accs, cf, own_start, OWN)

    for i, w in enumerate(where):
        mixed = None
        for c in range(3):
            v = tan2[c * erow + i * 8 : c * erow + i * 8 + 8, :] * (tacc[i][c + 1] + hacc[i][c + 1])
            mixed = v if mixed is None else mixed + v
        out_ref[w, :] = scale[w, :] * res[w, :] + ((hacc[i][0] - tacc[i][0]) + 0.5 * mixed)

    pl.when(g != G - 1)(parts_left)
    left(part_rows(psend, FAR), 9)
    left(got_send, 1)

    @pl.when(seam)
    def _():
        left(cf, 2)
        left(sq, 3)

    @pl.when(either_aide)
    def _():
        left(relay_p, 10)
        left(relay_l, 11)

    for rnd in range(SWEEPS):
        counts = ((inner, 4), (feeds, 5), (seam, 6)) if rnd % 2 == 0 else ((plain, 4), (seam, 3))
        for which, n in counts:
            pl.when(which)(lambda n=n: left(tab.at[rnd, pl.ds(0, n * vrow)], 4 + rnd))


def body(
    residual, edge_scale, tangent, edge_tail, edge_head,
    stencil_index, stencil_coef, diag_margin, send_index,
):
    edges = residual.shape[0]
    erow = edges // LANES
    nodes = diag_margin.shape[1]
    nrow = nodes // LANES
    vrow = 4 * nrow
    stencil = stencil_index.shape[0]
    qrow = -(-stencil * nrow // 8) * 8
    assert send_index.shape == (2, 2, nodes) and lax.axis_size("grp") % 2 == 0 and lax.axis_size("grp") > 4 and lax.axis_size("sub") % 2 == 0
    coef = jnp.transpose(stencil_coef, (1, 0, 2))
    square = lambda x: x.reshape(erow, LANES)
    anyspace = pl.BlockSpec(memory_space=pl.ANY)
    vm = pltpu.VMEM
    dma = pltpu.SemaphoreType.DMA
    out = pl.pallas_call(
        kernel,
        out_shape=vm((erow, LANES), F32),
        in_specs=[anyspace] * 9,
        out_specs=pl.BlockSpec(memory_space=vm),
        scratch_shapes=[
            vm((erow, LANES), F32),
            vm(tangent.shape, F32),
            vm((erow, LANES), I32),
            vm((erow, LANES), I32),
            vm(stencil_index.shape, I32),
            vm(coef.shape, BF16),
            vm(diag_margin.shape, F32),
            vm(send_index.shape, I32),
            vm((erow, LANES), F32),
            vm((4,) + send_index.shape, I32),
            vm((8 * vrow, LANES), F32),
            vm((8 * vrow, LANES), F32),
            vm((SWEEPS, SLOTS * vrow, LANES), F32),
            vm((LANES, edges), BF16),
            vm((2 * vrow, edges), BF16),
            vm((4 * vrow, edges), BF16),
            vm((14 * vrow, edges), BF16),
            vm((LANES, 4 * nodes), BF16),
            vm((2 * vrow, 4 * nodes), BF16),
            vm((4 * vrow, LANES), F32),
            vm((4, qrow, LANES), F32),
            vm((4, qrow, LANES), F32),
            vm((vrow, LANES), F32),
            vm((vrow, LANES), F32),
            vm((erow, LANES), I32),
            vm((erow, LANES), I32),
            vm((qrow, LANES), I32),
            vm((qrow, LANES), I32),
            vm((qrow, LANES), I32),
            vm((4 * qrow, LANES), F32),
            vm((3 * erow, LANES), F32),
            vm((2 * vrow, LANES), F32),
            vm(send_index.shape, I32),
            dma((12,)),
            dma((8 + 9 * (SWEEPS // 2),)),
        ],
        compiler_params=pltpu.CompilerParams(collective_id=0, has_side_effects=True),
    )(
        square(residual), tangent, square(edge_tail), square(edge_head),
        stencil_index, coef, diag_margin, send_index, square(edge_scale),
    )
    return out.reshape(edges)


def solution(mesh):
    return jax.shard_map(
        body,
        mesh=mesh,
        in_specs=(
            P(("grp", "sub")),
            P(("grp", "sub")),
            P(None, ("grp", "sub")),
            P(("grp", "sub")),
            P(("grp", "sub")),
            P(None, ("grp", "sub")),
            P(None, None, ("grp", "sub")),
            P(None, ("grp", "sub")),
            P("grp", "sub", None),
        ),
        out_specs=P(("grp", "sub")),
        check_vma=False,
    )
```

```python
import jax
import jax.numpy as jnp
from jax import lax
from jax.experimental import pallas as pl
from jax.experimental.pallas import tpu as pltpu
from jax.sharding import PartitionSpec as P

SWEEPS = 4
LANES = 128
SLOTS = 8
MESH = pl.DeviceIdType.MESH
DNUMS = lax.GatherDimensionNumbers(
    offset_dims=(),
    collapsed_slice_dims=(1,),
    start_index_map=(1,),
    operand_batching_dims=(0,),
    start_indices_batching_dims=(0,),
)
F32 = jnp.float32
BF16 = jnp.bfloat16
I32 = jnp.int32

OWN, FAR, NEAR, SM, SP = range(5)
FAR_NEAR, FAR_SM, FAR_SP = 5, 6, 7
GHOST_SLOT = (FAR, OWN, FAR_NEAR, FAR_SM, FAR_SP)


def lane_gather(table, lane):
    return lax.gather(
        table,
        lane[..., None],
        DNUMS,
        slice_sizes=(1, 1),
        mode=lax.GatherScatterMode.PROMISE_IN_BOUNDS,
    )


def nt_dot(a, b):
    return lax.dot_general(a, b, (((1,), (1,)), ((), ())), preferred_element_type=F32)


def kernel(
    res_h, tan_h, tail_h, head_h, sidx_h, coef_h, marg_h, send_h, scale_h,
    out_ref,
    res, tan, tail, head, sidx, coef, marg, own_send, scale,
    got_send, psend, got_p, tab, onehot, spread_o, spread_f, spread_r, onehot3, spread3, tsum,
    cf, gcf, bsc, diag, hq, hl, sq, gq, sidx2, gacc, tan2, relay_p, relay_l,
    send_sem, recv_sem,
):
    G, S = lax.axis_size("grp"), lax.axis_size("sub")
    g, s = lax.axis_index("grp"), lax.axis_index("sub")
    odd = lax.rem(g, 2)
    even = 1 - odd
    gf, gn = lax.rem(g + G - 1 + 2 * odd, G), lax.rem(g + 1 + (G - 2) * odd, G)
    sm, sp = lax.rem(s + S - 1, S), lax.rem(s + 1, S)
    peer = {FAR: (gf, s), NEAR: (gn, s), SM: (g, sm), SP: (g, sp)}
    nn_to = (lax.rem(g + 2 + (G - 4) * odd, G), s)
    seam = (g == 0) | (g == G - 1)
    plain = (g != 0) & (g != G - 1)
    feeds = (g == 1) | (g == G - 2)
    inner = plain & (g != 1) & (g != G - 2)
    s_odd = lax.rem(s, 2)
    paired = (g, s + 1 - 2 * s_odd)
    lead = (g == 0) & (s_odd == 0)
    led = (g != 0) | (s_odd != 0)
    aide = (g == 0) & (s_odd == 1)
    far_aide = (g == G - 1) & (s_odd == 1)
    either_aide = seam & (s_odd == 1)
    back = {FAR: FAR, NEAR: NEAR, SM: SP, SP: SM}
    nrow = marg.shape[1] // LANES
    erow = res.shape[0]
    stencil = sidx.shape[0]
    vrow = 4 * nrow
    sent = 2 * vrow
    tiles = [slice(i * 8, i * 8 + 8) for i in range(sq.shape[0] // 8)]

    barrier = pltpu.get_barrier_semaphore()
    skip = (g == G - 1) & (s_odd == 0)
    greeted = (jnp.where(skip, lax.rem(g + 2, G), gf), s)
    for who in (greeted, peer[NEAR], peer[SM], peer[SP]):
        pl.semaphore_signal(barrier, inc=1, device_id=who, device_id_type=MESH)

    pairs = (
        (head_h, head, 0), (res_h, res, 4), (tan_h, tan, 5), (send_h, own_send, 1), (tail_h, tail, 2),
        (coef_h, coef, 3), (marg_h, marg, 14), (sidx_h, sidx, 15), (scale_h, scale, 16),
    )
    local = [
        pltpu.make_async_copy(src, dst, send_sem.at[i] if i < 14 else recv_sem.at[i]) for src, dst, i in pairs
    ]
    for c in local:
        c.start()

    def copy_to(src, dst, ssem, rsem, who):
        return pltpu.make_async_remote_copy(
            src_ref=src, dst_ref=dst, send_sem=send_sem.at[ssem], recv_sem=recv_sem.at[rsem],
            device_id=who, device_id_type=MESH,
        )

    def landed(dst, rsem):
        copy_to(dst, dst, 0, rsem, peer[SP]).wait_recv()

    def left(src, ssem):
        copy_to(src, src, ssem, 0, peer[SP]).wait_send()

    def part_rows(ref, o):
        return ref.at[pl.ds((o - 1) * sent, sent)]

    def send_part(o):
        far = o == FAR
        copy_to(part_rows(psend, o), part_rows(got_p, back[o]), 5 if far else 0, 0 if far else 1, peer[o]).start()

    def send_list(o):
        copy_to(own_send, got_send.at[back[o] - 1], 1, 23 if o == FAR else 2, peer[o]).start()

    def slot_rows(rnd, slot):
        return tab.at[rnd, pl.ds(slot * vrow, vrow)]

    def table_sem(rnd, slot):
        slot = min(slot, FAR_NEAR) if isinstance(slot, int) else slot
        return 5 + 9 * (rnd // 2) + slot - 1 + FAR_NEAR * (rnd % 2)

    def send_table(rnd, who, slot):
        copy_to(slot_rows(rnd, OWN), slot_rows(rnd, slot), 4, table_sem(rnd, slot), who).start()

    def table_here(rnd, first, count=1):
        landed(tab.at[rnd, pl.ds(first * vrow, count * vrow)], table_sem(rnd, first))

    riota = lax.broadcasted_iota(I32, (vrow, LANES), 0)
    kind = riota // nrow
    rpart = (riota - kind * nrow).astype(F32).astype(BF16)
    lane16 = lax.broadcasted_iota(I32, (16, LANES), 0).astype(F32).astype(BF16)
    one, zero = jnp.ones((), BF16), jnp.zeros((), BF16)

    def cols_of(t):
        return slice(t * LANES, (t + 1) * LANES)

    def wide(row, rows):
        return jnp.broadcast_to(row.astype(F32), (rows, LANES)).astype(BF16)

    def lanes_onehot(ref, cols, x):
        lane = wide(x & (LANES - 1), 16)
        for q in range(LANES // 16):
            mine = lane16 + jnp.full((), 16 * q, BF16)
            ref[q * 16 : q * 16 + 16, cols] = jnp.where(mine == lane, one, zero)

    def split(val):
        hi = val.astype(BF16)
        return hi, (val - hi.astype(F32)).astype(BF16)

    def terms(t, sign):
        r = res[t : t + 1, :]
        val = jnp.broadcast_to(r if sign > 0 else -r, (vrow, LANES))
        half = 0.5 * r
        for c in range(3):
            val = jnp.where(kind == c + 1, tan[c : c + 1, cols_of(t)] * half, val)
        return split(val)

    def scatter(ref, rows_of, bases, sign, make=None):
        n = len(bases)
        for t in range(erow):
            cols = cols_of(t)
            x = rows_of[t : t + 1, :]
            if make:
                lanes_onehot(onehot, cols, x)
            pieces = terms(t, sign)
            row = wide(x >> 7, vrow)
            for j, base in enumerate(bases):
                hit = row == rpart + base
                for p, v in enumerate(pieces):
                    at = (p * n + j) * vrow
                    ref[at : at + vrow, cols] = jnp.where(hit, v, zero)
        both = nt_dot(ref[...], onehot[...])
        return both[: n * vrow] + both[n * vrow :]

    def base_of(block):
        return (jnp.asarray(block, I32) * nrow).astype(F32).astype(BF16)

    far_block, near_block = 1 + 2 * odd, 3 - 2 * odd

    for c in local[:4]:
        c.wait()
    psend[0:sent] = scatter(spread_f, head, [base_of(far_block), base_of(far_block + 1)], 1, make=True)

    extra = (g == 1) & (s_odd == 0)

    def first_sends():
        pl.semaphore_wait(barrier, jnp.where(lead, 3, jnp.where(extra, 5, 4)))

        @pl.when(lead)
        def _():
            copy_to(part_rows(psend, FAR), relay_p, 5, 10, paired).start()
            copy_to(own_send, relay_l, 1, 19, paired).start()

        @pl.when(aide)
        def _():
            landed(relay_p, 10)
            copy_to(relay_p, relay_p, 6, 10, peer[FAR]).start()
            landed(relay_l, 19)
            copy_to(relay_l, relay_l, 7, 19, peer[FAR]).start()

        @pl.when(led)
        def _():
            send_part(FAR)
            send_list(FAR)

        for o in (NEAR, SM, SP):
            send_list(o)

    late = (g == 0) | extra
    pl.when(jnp.logical_not(late))(first_sends)
    rest = scatter(
        spread_r, head,
        [base_of(b) for b in (near_block, near_block + 1, 5, 6, 7, 8, 0)], 1,
    )
    psend[sent:] = rest[: 3 * sent]
    own_sum = rest[3 * sent :]
    pl.when(late)(first_sends)
    for o in (NEAR, SM, SP):
        send_part(o)
    for c in local[4:]:
        c.wait()

    if cf.shape[1] > stencil * nrow:
        cf[...] = jnp.zeros_like(cf)
        sidx2[...] = jnp.zeros_like(sidx2)
    for k in range(4):
        for r in range(nrow):
            cols = cols_of(r)
            c = coef[:, k, cols].astype(F32)
            d = (1.0 + marg[k : k + 1, cols]) * jnp.sum(jnp.abs(c), axis=0, keepdims=True)
            inv = 1.0 / d
            diag[k * nrow + r : k * nrow + r + 1, :] = inv
            cf[k, pl.ds(r, stencil, stride=nrow), :] = c * inv

    for t in range(erow):
        lanes_onehot(onehot, cols_of(t), tail[t : t + 1, :])
    own_sum = own_sum + scatter(spread_o, tail, [base_of(0)], -1)

    a_of = (odd, even)
    lists = tuple((f, b, r) for f in range(2) for b in range(2) for r in range(nrow))

    def own_list(f, b, r):
        return own_send[a_of[f], b : b + 1, cols_of(r)]

    for n, fbr in enumerate(lists):
        lanes_onehot(onehot3, cols_of(n), own_list(*fbr))
    for c in range(3):
        for t in range(erow):
            tan2[c * erow + t : c * erow + t + 1, :] = tan[c : c + 1, cols_of(t)]
    for r in range(nrow):
        sidx2[pl.ds(r, stencil, stride=nrow), :] = sidx[:, cols_of(r)]

    def place(ref, at, f, b, r):
        hit = wide(own_list(f, b, r) >> 7, vrow) == rpart
        base = b * vrow + r + at
        val = jnp.broadcast_to(ref[base : base + 1, :], (vrow, LANES))
        for k in range(1, 4):
            row = base + k * nrow
            val = jnp.where(kind == k, ref[row : row + 1, :], val)
        return [jnp.where(hit, v, zero) for v in split(val)]

    parts_left = lambda: left(psend.at[pl.ds(sent, 3 * sent)], 0)
    pl.when(g == G - 1)(parts_left)

    def send_factor():
        copy_to(cf, gcf, 2, 3, peer[FAR]).start()

    pl.when(seam & led)(send_factor)

    @pl.when(far_aide)
    def _():
        landed(relay_p, 10)
        copy_to(relay_p, part_rows(got_p, FAR), 6, 0, paired).start()
        landed(relay_l, 19)
        copy_to(relay_l, got_send.at[FAR - 1], 7, 23, paired).start()

    def compose(x, y, parts):
        lane = x & (LANES - 1)
        row = x >> 7
        for o in parts:
            block = {FAR: far_block, NEAR: near_block, SM: 5, SP: 7}[o]
            for h in range(2):
                a, b = {FAR: (even, h), NEAR: (odd, h), SM: (h, 1), SP: (h, 0)}[o]
                for r in range(nrow):
                    line = got_send[o - 1, a, b : b + 1, cols_of(r)]
                    line = jnp.broadcast_to(line + o * nrow * LANES, x.shape)
                    y = jnp.where(row == (block + h) * nrow + r, lane_gather(line, lane), y)
        return y

    landed(got_send.at[pl.ds(NEAR - 1, 3)], 2)
    for w in tiles:
        sq[w, :] = compose(sidx2[w, :], sidx2[w, :], (NEAR, SM, SP))

    landed(got_p.at[pl.ds(sent, 3 * sent)], 1)
    for f in range(2):
        for b in range(2):
            first = pl.multiple_of((2 + b) * sent + a_of[f] * vrow, vrow)
            val = got_p[pl.ds(first, vrow), :]
            if f:
                val = val + got_p[sent + b * vrow : sent + (b + 1) * vrow, :]
            at = (f * 2 + b) * vrow
            tsum[at : at + vrow, :] = val
    for n, (f, b, r) in enumerate(lists):
        for p, v in enumerate(place(tsum, f * sent, f, b, r)):
            spread3[p * vrow : (p + 1) * vrow, cols_of(n)] = v
    got = nt_dot(spread3[...], onehot3[...])
    own_sum = own_sum + (got[:vrow] + got[vrow:])

    landed(part_rows(got_p, FAR), 0)
    half = len(lists) // 2
    for n, (f, b, r) in enumerate(lists[:half]):
        for p, v in enumerate(place(got_p, 0, f, b, r)):
            spread3[p * vrow : (p + 1) * vrow, cols_of(n)] = v
    got = nt_dot(spread3[:, : half * LANES], onehot3[:, : half * LANES])
    bsc[...] = (own_sum + (got[:vrow] + got[vrow:])) * diag[...]
    tab[0, :vrow, :] = bsc[...]

    def send_round(rnd, deep):
        if deep:
            send_table(rnd, peer[FAR], FAR)
        for o in (NEAR, SM, SP):
            send_table(rnd, peer[o], back[o])
        if deep:
            @pl.when(seam)
            def _():
                send_table(rnd, (gf, sp), FAR_SM)
                send_table(rnd, (gf, sm), FAR_SP)

            @pl.when(feeds)
            def _():
                send_table(rnd, nn_to, FAR_NEAR)
        else:
            @pl.when(plain)
            def _():
                send_table(rnd, peer[FAR], FAR)

    def compose_far():
        landed(got_send.at[FAR - 1], 23)
        for w in tiles:
            sq[w, :] = compose(sidx2[w, :], sq[w, :], (FAR,))

        @pl.when(seam)
        def _():
            copy_to(sq, gq, 3, 4, peer[FAR]).start()

        pl.when(lead)(send_factor)

    def compose_heads():
        for i in range(erow // 8):
            x = head[i * 8 : i * 8 + 8, :]
            y = compose(x, x, (FAR, NEAR, SM, SP))
            hq[i * 8 : i * 8 + 8, :] = y >> 7
            hl[i * 8 : i * 8 + 8, :] = y & (LANES - 1)

    def add_rows(rnd, slot, part, rows, lanes, accs):
        for i in range(len(rows)):
            for r in range(nrow):
                hit = rows[i] == part * nrow + r
                for k in range(4):
                    at = slot * vrow + k * nrow + r
                    line = jnp.broadcast_to(tab[rnd, pl.ds(at, 1), :], rows[i].shape)
                    v = lane_gather(line, lanes[i])
                    accs[i][k] = v if accs[i][k] is None else jnp.where(hit, v, accs[i][k])

    sub8 = lax.broadcasted_iota(I32, (8, LANES), 0)

    def open_sweep(rnd, index):
        where = [index[w, :] for w in tiles]
        rows = [y >> 7 for y in where]
        lanes = [y & (LANES - 1) for y in where]
        accs = [[None] * 4 for _ in tiles]

        def add(part, slot=None):
            add_rows(rnd, part if slot is None else slot, part, rows, lanes, accs)

        return add, accs

    def close_sweep(rnd, accs, factor, start, out_slot):
        totals = []
        for k in range(4):
            total = None
            for w, acc in zip(tiles, accs):
                v = acc[k] * factor[k, w, :]
                total = v if total is None else total + v
            step = nrow
            while step < 8:
                total = total + pltpu.roll(total, step, axis=0)
                step *= 2
            totals.append(total)
        for at in range(0, vrow, 8):
            total = totals[at // nrow]
            for m in range(1, 8 // nrow):
                total = jnp.where(sub8 >= m * nrow, totals[at // nrow + m], total)
            to = out_slot * vrow + at
            tab[rnd + 1, to : to + 8, :] = start(at) - total

    def own_start(at):
        return bsc[at : at + 8, :]

    def ghost_start(at):
        return tab[0, FAR * vrow + at : FAR * vrow + at + 8, :]

    partner, across = SP - s_odd, SM + s_odd
    second, third = SM - s_odd, NEAR + 2 * s_odd

    def either(here, there):
        return [jnp.where(seam, a, b) for a, b in zip(here, there)]

    slow_order = (
        either((partner, second, third, FAR), (partner, across, FAR, NEAR)),
        either((partner, second, third, FAR), (partner, across, NEAR, FAR)),
    )
    late_order = either((partner, second, third, FAR), (partner, across, FAR, NEAR))
    early_order = either((FAR, partner, second, third), (partner, across, FAR, NEAR))

    for rnd in range(0, SWEEPS, 2):
        send_round(rnd, True)
        if rnd == 0:
            compose_far()
            compose_heads()
        add, accs = open_sweep(rnd, sq)
        add(OWN)
        for part in slow_order[rnd // 2]:
            table_here(rnd, part)
            add(part)
        close_sweep(rnd, accs, cf, own_start, OWN)
        send_round(rnd + 1, False)

        final = rnd + 2 == SWEEPS
        if final:
            where = [slice(i * 8, i * 8 + 8) for i in range(erow // 8)]
            tails = [tail[w, :] for w in where]
            tacc = [[None] * 4 for _ in where]
            add_rows(rnd + 1, OWN, OWN, [t >> 7 for t in tails], [t & (LANES - 1) for t in tails], tacc)
            rows = [hq[w, :] for w in where]
            lanes = [hl[w, :] for w in where]
            hacc = [[None] * 4 for _ in where]

            def add(part):
                add_rows(rnd + 1, part, part, rows, lanes, hacc)
        else:
            add, accs = open_sweep(rnd + 1, sq)
        add(OWN)

        def ghost_tables():
            if rnd == 0:
                landed(gq, 4)
            ghost_add, ghost_accs = open_sweep(rnd, gq)
            ghost_add(OWN, FAR)
            ghost_add(FAR, OWN)
            table_here(rnd, FAR_NEAR, 3)
            for part in (NEAR, SM, SP):
                ghost_add(part, GHOST_SLOT[part])
            return ghost_accs

        def ghost_begin():
            for n, v in enumerate(sum(ghost_tables(), [])):
                gacc[n * 8 : n * 8 + 8, :] = v

        def ghost_end():
            landed(gcf, 3)
            held = [[gacc[n * 8 : n * 8 + 8, :] for n in range(4 * i, 4 * i + 4)] for i in range(len(tiles))]
            close_sweep(rnd, held, gcf, ghost_start, FAR)

        def ghost_whole():
            close_sweep(rnd, ghost_tables(), gcf, ghost_start, FAR)

        if not final:
            pl.when(seam)(ghost_begin)
            for n, part in enumerate(late_order):
                if n < 3:
                    table_here(rnd + 1, part)
                else:
                    pl.when(seam)(ghost_end)
                    pl.when(plain)(lambda: table_here(rnd + 1, NEAR))
                add(part)
        else:
            pl.when(seam)(ghost_whole)
            pl.when(plain)(lambda: table_here(rnd + 1, partner))
            for n, part in enumerate(early_order):
                if n:
                    table_here(rnd + 1, part)
                add(part)
        if not final:
            close_sweep(rnd + 1, accs, cf, own_start, OWN)

    for i, w in enumerate(where):
        mixed = None
        for c in range(3):
            v = tan2[c * erow + i * 8 : c * erow + i * 8 + 8, :] * (tacc[i][c + 1] + hacc[i][c + 1])
            mixed = v if mixed is None else mixed + v
        out_ref[w, :] = scale[w, :] * res[w, :] + ((hacc[i][0] - tacc[i][0]) + 0.5 * mixed)

    pl.when(g != G - 1)(parts_left)
    left(part_rows(psend, FAR), 5)
    left(got_send, 1)

    @pl.when(seam)
    def _():
        left(cf, 2)
        left(sq, 3)

    @pl.when(either_aide)
    def _():
        left(relay_p, 6)
        left(relay_l, 7)

    pl.when(inner)(lambda: left(tab.at[pl.ds(0, 2)], 4))
    pl.when(jnp.logical_not(inner))(lambda: left(tab.at[pl.ds(0, 3), pl.ds(0, 6 * vrow)], 4))


def body(
    residual, edge_scale, tangent, edge_tail, edge_head,
    stencil_index, stencil_coef, diag_margin, send_index,
):
    edges = residual.shape[0]
    erow = edges // LANES
    nodes = diag_margin.shape[1]
    nrow = nodes // LANES
    vrow = 4 * nrow
    stencil = stencil_index.shape[0]
    qrow = -(-stencil * nrow // 8) * 8
    assert send_index.shape == (2, 2, nodes) and lax.axis_size("grp") % 2 == 0 and lax.axis_size("grp") > 4 and lax.axis_size("sub") % 2 == 0
    coef = jnp.transpose(stencil_coef, (1, 0, 2))
    square = lambda x: x.reshape(erow, LANES)
    anyspace = pl.BlockSpec(memory_space=pl.ANY)
    vm = pltpu.VMEM
    dma = pltpu.SemaphoreType.DMA
    out = pl.pallas_call(
        kernel,
        out_shape=vm((erow, LANES), F32),
        in_specs=[anyspace] * 9,
        out_specs=pl.BlockSpec(memory_space=vm),
        scratch_shapes=[
            vm((erow, LANES), F32),
            vm(tangent.shape, F32),
            vm((erow, LANES), I32),
            vm((erow, LANES), I32),
            vm(stencil_index.shape, I32),
            vm(coef.shape, BF16),
            vm(diag_margin.shape, F32),
            vm(send_index.shape, I32),
            vm((erow, LANES), F32),
            vm((4,) + send_index.shape, I32),
            vm((8 * vrow, LANES), F32),
            vm((8 * vrow, LANES), F32),
            vm((SWEEPS, SLOTS * vrow, LANES), F32),
            vm((LANES, edges), BF16),
            vm((2 * vrow, edges), BF16),
            vm((4 * vrow, edges), BF16),
            vm((14 * vrow, edges), BF16),
            vm((LANES, 4 * nodes), BF16),
            vm((2 * vrow, 4 * nodes), BF16),
            vm((4 * vrow, LANES), F32),
            vm((4, qrow, LANES), F32),
            vm((4, qrow, LANES), F32),
            vm((vrow, LANES), F32),
            vm((vrow, LANES), F32),
            vm((erow, LANES), I32),
            vm((erow, LANES), I32),
            vm((qrow, LANES), I32),
            vm((qrow, LANES), I32),
            vm((qrow, LANES), I32),
            vm((4 * qrow, LANES), F32),
            vm((3 * erow, LANES), F32),
            vm((2 * vrow, LANES), F32),
            vm(send_index.shape, I32),
            dma((8,)),
            dma((6 + 9 * (SWEEPS // 2),)),
        ],
        compiler_params=pltpu.CompilerParams(collective_id=0, has_side_effects=True),
    )(
        square(residual), tangent, square(edge_tail), square(edge_head),
        stencil_index, coef, diag_margin, send_index, square(edge_scale),
    )
    return out.reshape(edges)


def solution(mesh):
    return jax.shard_map(
        body,
        mesh=mesh,
        in_specs=(
            P(("grp", "sub")),
            P(("grp", "sub")),
            P(None, ("grp", "sub")),
            P(("grp", "sub")),
            P(("grp", "sub")),
            P(None, ("grp", "sub")),
            P(None, None, ("grp", "sub")),
            P(None, ("grp", "sub")),
            P("grp", "sub", None),
        ),
        out_specs=P(("grp", "sub")),
        check_vma=False,
    )
```
